128 devices in a mesh: gx: 16 (over z, x), gy: 8 (over y, core).
Axes of the slice: x: 4, y: 4, z: 4, core: 2. Of those that a mesh axis runs over, the one named last changes fastest.
Arguments:
- pressure: float32 [10, 1024, 4096], P(None, 'gx', 'gy'), may hold values from -6 to 6
- pressure_old: float32 [10, 1024, 4096], P(None, 'gx', 'gy'), may hold values from -6 to 6
- conductivity: float32 [10, 1024, 4096], P(None, 'gx', 'gy'), may hold values from 0.1 to 1
- porosity: float32 [10, 1024, 4096], P(None, 'gx', 'gy'), may hold values from 2 to 8
- recharge: float32 [1024, 4096], P('gx', 'gy'), may hold values from -6 to 6
- active: int32 [1024, 4096], P('gx', 'gy'), may hold values from 0 to 1, as said below
Outputs:
- final_pressure: float32 [10, 1024, 4096], P(None, 'gx', 'gy')
- linear_residual: float32 [10, 1024, 4096], P(None, 'gx', 'gy')
The draws below stay inside these ranges and needn't reach their ends.
Inputs may be any that keep to these rules, and one draw needn't show every extreme that they name: `active`: 1 marks a land column, 0 an ocean column.
All inputs are finite; a program needn't handle non-finite values.
Results may differ from the reference program's by a relative error of at most 0.0003.
Values sent between devices are 32-bit elements; how exact they have to be, the bound alone decides.
No kernel may reach another device: no remote copies, remote signals or barrier semaphores. Data moves between devices by JAX's collectives and lax.ppermute only.
A program may use at most 128 MiB of HBM per device.

```python
import math
import jax
import jax.numpy as jnp

CX = 64
CY = 512
NZ = 10
STEPS = 1
NEWTON = 2
NX = 1024
NY = 4096


def draw_active(key, part):
    key_corner = jax.random.fold_in(key, 11)
    key_jitter = jax.random.fold_in(key, 12)
    tiles_x = NX // CX
    tiles_y = NY // CY
    corners = jax.random.randint(key_corner, (tiles_x + 1, tiles_y + 1), 0, 10, dtype=jnp.int32)
    row_index = jnp.arange(NX, dtype=jnp.int32)
    row_tile = row_index // CX
    row_frac = row_index % CX
    blended = corners[row_tile] * (CX - row_frac)[:, None] + corners[row_tile + 1] * row_frac[:, None]
    column_index = jnp.arange(NY, dtype=jnp.int32)
    column_tile = column_index // CY
    column_frac = column_index % CY
    surface = blended[:, column_tile] * (CY - column_frac)[None] + blended[:, column_tile + 1] * column_frac[None]
    jitter = jax.random.randint(key_jitter, (NX, NY), 0, 3 * CX * CY, dtype=jnp.int32)
    land_mask = jnp.where(surface + jitter > 6 * CX * CY, 1, 0).astype(jnp.int32)
    land_mask = land_mask.at[0, 0].set(1)
    land_mask = land_mask.at[0, 1].set(0)
    return land_mask


def levels(rng, shape, pieces, least, top_value):
    gain, own = 1.0, jax.random.fold_in(rng, 6)
    for axis_at, parts in pieces:
        steps = jnp.exp(jax.random.uniform(jax.random.fold_in(own, axis_at), (parts,), jnp.float32, least / len(pieces), top_value / len(pieces)))
        gain = gain * jnp.repeat(steps, shape[axis_at] // parts).reshape([-1 if axis == axis_at else 1 for axis in range(len(shape))])
    return gain


def normal_values(stream_key, extent, deviation, most, pieces=(), kind=jnp.bfloat16):
    gain = levels(stream_key, extent, pieces, -0.22, 0.18) if pieces else 1.0
    result = jax.random.normal(stream_key, extent, jnp.float32) * deviation * gain
    return jnp.minimum(jnp.maximum(result, -most), most).astype(kind)


def setup_inputs(seed: int = 0) -> dict:
    streams_of = jax.random.split(jax.random.key(seed), 7)
    pressure = normal_values(streams_of[0], (NZ, NX, NY), 1.0, 6.0, ((1, 16), (2, 8)), jnp.float32)
    pressure_old = normal_values(streams_of[1], (NZ, NX, NY), 1.0, 6.0, ((1, 16), (2, 8)), jnp.float32)
    conductivity = jnp.clip(jnp.exp(math.log(1.0) - 2.3025851 * jax.random.uniform(streams_of[2], (NZ, NX, NY), jnp.float32) ** levels(streams_of[2], (NZ, NX, NY), ((1, 16), (2, 8)), -0.2, 0.2)), 0.1, 1.0)
    porosity = jnp.clip(jnp.exp(math.log(8.0) - 1.3862944 * jax.random.uniform(streams_of[3], (NZ, NX, NY), jnp.float32) ** levels(streams_of[3], (NZ, NX, NY), ((1, 16), (2, 8)), -0.2, 0.2)), 2.0, 8.0)
    recharge = normal_values(streams_of[4], (NX, NY), 1.0, 6.0, ((0, 16), (1, 8)), jnp.float32)
    active = draw_active(jax.random.fold_in(streams_of[6], 71), 0)
    return dict(pressure=pressure, pressure_old=pressure_old, conductivity=conductivity, porosity=porosity, recharge=recharge, active=active)


residual_sat = 0.1
vertical_factor = 2.0
epsilon = 1e-06

def interior(array):
    return array[:, 1:-1, 1:-1]

def saturation(values):
    return residual_sat + (1.0 - residual_sat) * jax.nn.sigmoid(values)

def sat_slope(values):
    sigma = jax.nn.sigmoid(values)
    return (1.0 - residual_sat) * sigma * (1.0 - sigma)

def face_pair(press_low, press_high, cond_low, cond_high, act_low, act_high, factor, gravity):
    transmit = 0.5 * factor * (cond_low + cond_high) * act_low * act_high
    sig_low = jax.nn.sigmoid(press_low)
    sig_high = jax.nn.sigmoid(press_high)
    mobility = 0.5 * (sig_low * sig_low + sig_high * sig_high)
    head_drop = press_low - press_high + gravity
    coef_low = transmit * (mobility + sig_low * sig_low * (1.0 - sig_low) * head_drop)
    coef_high = transmit * (sig_high * sig_high * (1.0 - sig_high) * head_drop - mobility)
    return (coef_low, coef_high, transmit * mobility * head_drop)

def coefficients(pressure, conduct, active):
    across_x = face_pair(pressure[:, :-1, 1:-1], pressure[:, 1:, 1:-1], conduct[:, :-1, 1:-1], conduct[:, 1:, 1:-1], active[:, :-1, 1:-1], active[:, 1:, 1:-1], 1.0, 0.0)
    across_y = face_pair(pressure[:, 1:-1, :-1], pressure[:, 1:-1, 1:], conduct[:, 1:-1, :-1], conduct[:, 1:-1, 1:], active[:, 1:-1, :-1], active[:, 1:-1, 1:], 1.0, 0.0)
    inner_p = interior(pressure)
    inner_k = interior(conduct)
    inner_a = interior(active)
    across_z = face_pair(inner_p[:-1], inner_p[1:], inner_k[:-1], inner_k[1:], inner_a[:-1], inner_a[1:], vertical_factor, -1.0)
    return (across_x, across_y, across_z)

def outflow(flow_x, flow_y, flow_z):
    total = flow_x[:, 1:] - flow_x[:, :-1] + flow_y[:, :, 1:] - flow_y[:, :, :-1]
    zeros = jnp.zeros_like(flow_z[:1])
    return total + jnp.concatenate([flow_z, zeros], 0) - jnp.concatenate([zeros, flow_z], 0)

def jacobian_apply(vector, faces, diagonal, active):
    x_low, x_high, x_flow = faces[0]
    y_low, y_high, y_flow = faces[1]
    z_low, z_high, z_flow = faces[2]
    flow_x = x_low * vector[:, :-1, 1:-1] + x_high * vector[:, 1:, 1:-1]
    flow_y = y_low * vector[:, 1:-1, :-1] + y_high * vector[:, 1:-1, 1:]
    center = interior(vector)
    flow_z = z_low * center[:-1] + z_high * center[1:]
    return active * (diagonal * center + outflow(flow_x, flow_y, flow_z)) + (1.0 - active) * center

def newton_residual(pressure, faces, pressure_old, porosity, recharge, active):
    center = interior(pressure)
    storage = porosity * (saturation(center) - saturation(pressure_old))
    inflow = jnp.concatenate([jnp.zeros_like(center[:-1]), recharge[None]], 0)
    flows = outflow(faces[0][2], faces[1][2], faces[2][2])
    return active * (storage - inflow + flows) + (1.0 - active) * center

def least_squares(first_norm, entry_one, entry_two, entry_three, entry_four, entry_five):
    radius = jnp.sqrt(entry_one * entry_one + entry_two * entry_two)
    cosine = entry_one / radius
    sine = entry_two / radius
    top_right = cosine * entry_three + sine * entry_four
    lower = cosine * entry_four - sine * entry_three
    weight_two = -lower * sine * first_norm / (lower * lower + entry_five * entry_five)
    weight_one = (cosine * first_norm - top_right * weight_two) / radius
    return (weight_one, weight_two)

def widen(array):
    return jnp.pad(array, ((0, 0), (1, 1), (1, 1)))

def reference(pressure, pressure_old, conductivity, porosity, recharge, active):
    active_cells = jnp.broadcast_to(active.astype(jnp.float32)[None], pressure.shape)
    cond_ext = widen(conductivity)
    active_ext = widen(active_cells)
    current = pressure
    previous = pressure_old
    leftover = jnp.zeros_like(pressure)
    for step_index in range(STEPS):
        for newton_index in range(NEWTON):
            current_ext = widen(current)
            faces = coefficients(current_ext, cond_ext, active_ext)
            remainder = -newton_residual(current_ext, faces, previous, porosity, recharge, active_cells)
            diagonal = porosity * sat_slope(current)
            first_norm = jnp.sqrt(jnp.sum(remainder * remainder) + epsilon)
            basis_one = remainder / first_norm
            image_one = jacobian_apply(widen(basis_one), faces, diagonal, active_cells)
            entry_one = jnp.sum(image_one * basis_one)
            ortho_one = image_one - entry_one * basis_one
            entry_two = jnp.sqrt(jnp.sum(ortho_one * ortho_one) + epsilon)
            basis_two = ortho_one / entry_two
            image_two = jacobian_apply(widen(basis_two), faces, diagonal, active_cells)
            entry_three = jnp.sum(image_two * basis_one)
            entry_four = jnp.sum(image_two * basis_two)
            ortho_two = image_two - entry_three * basis_one - entry_four * basis_two
            entry_five = jnp.sqrt(jnp.sum(ortho_two * ortho_two) + epsilon)
            weight_one, weight_two = least_squares(first_norm, entry_one, entry_two, entry_three, entry_four, entry_five)
            current = current + (weight_one * basis_one + weight_two * basis_two)
            leftover = remainder - weight_one * image_one - weight_two * image_two
        previous = current
    return (current, leftover)
```

```python
import jax
import jax.numpy as jnp
from jax import lax
from jax.experimental import pallas as pl
from jax.experimental.pallas import tpu as pltpu
from jax.sharding import Mesh
from jax.sharding import PartitionSpec as P

GX = ("gx_0", "gx_1")
GY = ("gy_0", "gy_1")
ALL = GX + GY

EPS = 1e-06
NT = 5
ROWS = 80
TOP = 8
F32 = jnp.float32


def lanes():
    return lax.broadcasted_iota(jnp.int32, (8, 128), 1)


def from_north(tiles):
    lane = lanes()
    turned = [pltpu.roll(tile, 127, 1) for tile in tiles]
    count = len(tiles)
    return [jnp.where(lane == 127, turned[(t + 1) % count], turned[t]) for t in range(count)]


def from_south(tiles):
    lane = lanes()
    turned = [pltpu.roll(tile, 1, 1) for tile in tiles]
    count = len(tiles)
    return [jnp.where(lane == 0, turned[(t - 1) % count], turned[t]) for t in range(count)]


def tile_of(ref, layer, t, start):
    return ref[layer, t, pl.ds(start, 8), :]


def tiles_of(ref, layer, start):
    return [tile_of(ref, layer, t, start) for t in range(NT)]


def flat_tiles(ref, start):
    return [ref[t, pl.ds(start, 8), :] for t in range(NT)]


UNITS = 25


def load_kernel(layers, par, p_in, k_in, o_in, r_in, rech_in, act_in,
                p_ref, k_ref, o_ref, r_ref, rech_ref, act_ref, send_a, send_b, act_int, sems):
    copies = []
    for order, t in enumerate((0, 3, 1, 2)):
        cols = pl.ds(128 * t, 128)
        for f, (src, dst) in enumerate(((p_in, p_ref), (k_in, k_ref), (o_in, o_ref), (r_in, r_ref))):
            copies.append(pltpu.make_async_copy(
                src.at[:, :, cols], dst.at[:, t, pl.ds(TOP, 64), :], sems.at[order * 6 + f]))
        copies.append(pltpu.make_async_copy(
            rech_in.at[:, cols], rech_ref.at[t, pl.ds(TOP, 64), :], sems.at[order * 6 + 4]))
        copies.append(pltpu.make_async_copy(act_in.at[:, cols], act_int.at[t], sems.at[order * 6 + 5]))
    for copy in copies:
        copy.start()
    zero = jnp.zeros((8, 128), F32)

    def clear(layer, carry):
        for ref in (p_ref, k_ref, o_ref, r_ref):
            for t in range(NT):
                ref[layer, t, 0:8, :] = zero
                ref[layer, t, ROWS - 8:ROWS, :] = zero
        return carry

    lax.fori_loop(0, layers, clear, 0)
    for ref in (rech_ref, act_ref):
        for t in range(NT):
            ref[t, 0:8, :] = zero
            ref[t, ROWS - 8:ROWS, :] = zero
    for copy in copies[:12]:
        copy.wait()
    for t in (0, 3):
        act_ref[t, TOP:TOP + 64, :] = act_int[t].astype(F32)
    first = lanes() < 5
    last = lanes() >= 123
    odd = par[0] == 1

    def pack(row, carry):
        start = pl.multiple_of(TOP + 8 * row, 8)
        low = [zero, zero]
        high = [zero, zero]
        units = [(ref, layer) for ref in (p_ref, k_ref, o_ref, r_ref) for layer in range(layers)]
        units = units + [(act_ref, None), (rech_ref, None)]
        for u, (ref, layer) in enumerate(units):
            at = 5 * (u % UNITS)
            here = u // UNITS
            if layer is None:
                a, b = ref[0, pl.ds(start, 8), :], ref[3, pl.ds(start, 8), :]
            else:
                a, b = tile_of(ref, layer, 0, start), tile_of(ref, layer, 3, start)
            a = jnp.where(first, a, 0.0)
            b = jnp.where(last, b, 0.0)
            low[here] = low[here] + (pltpu.roll(a, at, 1) if at else a)
            high[here] = high[here] + pltpu.roll(b, (at + 5) % 128, 1)
        out = pl.multiple_of(8 * row, 8)
        for here in range(2):
            send_a[here, pl.ds(out, 8), :] = jnp.where(odd, low[here], high[here])
            send_b[here, pl.ds(out, 8), :] = jnp.where(odd, high[here], low[here])
        return carry

    lax.fori_loop(0, 8, pack, 0)
    for copy in copies[12:]:
        copy.wait()
    for t in (1, 2):
        act_ref[t, TOP:TOP + 64, :] = act_int[t].astype(F32)


def strip_rows(layers):
    return ((0, 5), (5, 5), (10, 4), (14, 4))


def turn_kernel(layers, par_y, par_x, p_old, k_old, o_old, r_old, rech_old, act_old, got_a, got_b,
                p_ref, k_ref, o_ref, r_ref, rech_ref, act_ref, send_a, send_b):
    odd = par_y[0] == 1
    left_edge = lanes() >= 123
    right_edge = lanes() < 5

    def unpack(row, carry):
        start = pl.multiple_of(TOP + 8 * row, 8)
        src = pl.multiple_of(8 * row, 8)
        a = [got_a[here, pl.ds(src, 8), :] for here in range(2)]
        b = [got_b[here, pl.ds(src, 8), :] for here in range(2)]
        below = [jnp.where(odd, a[h], b[h]) for h in range(2)]
        above = [jnp.where(odd, b[h], a[h]) for h in range(2)]
        units = [(ref, layer) for ref in (p_ref, k_ref, o_ref, r_ref) for layer in range(layers)]
        units = units + [(act_ref, None), (rech_ref, None)]
        for u, (ref, layer) in enumerate(units):
            at = 5 * (u % UNITS)
            here = u // UNITS
            left = pltpu.roll(below[here], (123 - at) % 128, 1)
            right = pltpu.roll(above[here], (128 - at) % 128, 1) if at else above[here]
            value = jnp.where(left_edge, left, jnp.where(right_edge, right, 0.0))
            if layer is None:
                ref[4, pl.ds(start, 8), :] = value
            else:
                ref[layer, 4, pl.ds(start, 8), :] = value
        return carry

    lax.fori_loop(0, 8, unpack, 0)
    up = par_x[0] == 1
    low, high = TOP, TOP + 64
    fields = (p_ref, k_ref, o_ref, r_ref)
    for send, lower in ((send_a, up), (send_b, jnp.logical_not(up))):
        start5 = jnp.where(lower, low, high - 5)
        start4 = jnp.where(lower, low, high - 4)

        def fill(layer, carry):
            for (at, depth), ref in zip(strip_rows(layers), fields):
                start = start5 if depth == 5 else start4
                for t in range(NT):
                    send[t, pl.ds(layer * 18 + at, depth), :] = ref[layer, t, pl.ds(start, depth), :]
            return carry

        lax.fori_loop(0, layers, fill, 0)
        for t in range(NT):
            send[t, 18 * layers:18 * layers + 5, :] = act_ref[t, pl.ds(start5, 5), :]
            send[t, 18 * layers + 5:18 * layers + 9, :] = rech_ref[t, pl.ds(start4, 4), :]


def place_strips(layers, up, refs, got_a, got_b):
    p_ref, k_ref, o_ref, r_ref, rech_ref, act_ref = refs
    fields = (p_ref, k_ref, o_ref, r_ref)
    low, high = TOP, TOP + 64
    for got, above in ((got_a, jnp.logical_not(up)), (got_b, up)):
        dst5 = jnp.where(above, high, low - 5)
        dst4 = jnp.where(above, high, low - 4)

        def fill(layer, carry):
            for (at, depth), ref in zip(strip_rows(layers), fields):
                start = dst5 if depth == 5 else dst4
                for t in range(NT):
                    ref[layer, t, pl.ds(start, depth), :] = got[t, pl.ds(layer * 18 + at, depth), :]
            return carry

        lax.fori_loop(0, layers, fill, 0)
        for t in range(NT):
            act_ref[t, pl.ds(dst5, 5), :] = got[t, 18 * layers:18 * layers + 5, :]
            rech_ref[t, pl.ds(dst4, 4), :] = got[t, 18 * layers + 5:18 * layers + 9, :]


def sigmoid_tile(value, layer, t, start, sig_ref, mob_ref, der_ref):
    sig = jax.nn.sigmoid(value)
    square = sig * sig
    sig_ref[layer, t, pl.ds(start, 8), :] = sig
    mob_ref[layer, t, pl.ds(start, 8), :] = 0.5 * square
    der_ref[layer, t, pl.ds(start, 8), :] = square - square * sig


def face(trans, p_a, p_b, m_a, m_b, s_a, s_b, gravity):
    drop = p_a - p_b
    if gravity:
        drop = drop + gravity
    by_mob = trans * (m_a + m_b)
    by_drop = trans * drop
    return by_mob + s_a * by_drop, s_b * by_drop - by_mob, by_mob * drop


def far_faces(layers, starts, s, make_trans):
    def one_layer(layer, carry):
        upper = jnp.minimum(layer + 1, layers - 1)
        inner = jnp.where(layer + 1 < layers, 1.0, 0.0).astype(F32)
        for start in starts:
            rows = pl.ds(start, 8)
            for t in range(NT):
                if make_trans:
                    trans = s.ax[t, rows, :] * (tile_of(s.k, layer, t, start) + tile_of(s.k, layer, t, start + 1))
                    s.tx[layer, t, rows, :] = trans
                else:
                    trans = tile_of(s.tx, layer, t, start)
                p = tile_of(s.p, layer, t, start)
                m = tile_of(s.m, layer, t, start)
                der = tile_of(s.s, layer, t, start)
                ca, cb, flow = face(
                    trans, p, tile_of(s.p, layer, t, start + 1), m, tile_of(s.m, layer, t, start + 1),
                    der, tile_of(s.s, layer, t, start + 1), 0.0)
                s.xa[layer, t, rows, :] = ca
                s.xb[layer, t, rows, :] = cb
                s.xf[layer, t, rows, :] = flow
                if make_trans:
                    trans = (s.act[t, rows, :] * inner) * (
                        tile_of(s.k, layer, t, start) + tile_of(s.k, upper, t, start))
                    s.tz[layer, t, rows, :] = trans
                else:
                    trans = tile_of(s.tz, layer, t, start)
                za, zb, zf = face(
                    trans, p, tile_of(s.p, upper, t, start), m, tile_of(s.m, upper, t, start),
                    der, tile_of(s.s, upper, t, start), -1.0)
                s.za[layer + 1, t, rows, :] = za
                s.zb[layer + 1, t, rows, :] = zb
                s.zf[layer + 1, t, rows, :] = zf
        return carry

    lax.fori_loop(0, layers, one_layer, 0)


def assemble(layers, starts, s, make_trans):
    def one_layer(layer, carry):
        for start in starts:
            rows = pl.ds(start, 8)
            p = tiles_of(s.p, layer, start)
            m = tiles_of(s.m, layer, start)
            der = tiles_of(s.s, layer, start)
            if make_trans:
                k = tiles_of(s.k, layer, start)
                k_north = from_north(k)
                ty = [s.ay[t, rows, :] * (k[t] + k_north[t]) for t in range(NT)]
                for t in range(NT):
                    s.ty[layer, t, rows, :] = ty[t]
            else:
                ty = tiles_of(s.ty, layer, start)
            p_north, m_north, s_north = from_north(p), from_north(m), from_north(der)
            across_y = [face(ty[t], p[t], p_north[t], m[t], m_north[t], der[t], s_north[t], 0.0) for t in range(NT)]
            ya = from_south([f[0] for f in across_y])
            yb = from_south([f[1] for f in across_y])
            yf = from_south([f[2] for f in across_y])
            for t in range(NT):
                s.ya[layer, t, rows, :] = ya[t]
                s.yb[layer, t, rows, :] = across_y[t][1]
                sig = tile_of(s.sig, layer, t, start)
                ap = tile_of(s.ap, layer, t, start)
                ocean = 1.0 - s.act[t, rows, :]
                stored = ap * sig
                center = (stored - stored * sig) + ocean
                center = center + (tile_of(s.xa, layer, t, start) - tile_of(s.xb, layer, t, start - 1))
                center = center + (across_y[t][0] - yb[t]) + (tile_of(s.za, layer + 1, t, start) - tile_of(s.zb, layer, t, start))
                s.c[layer, t, rows, :] = center
                flows = (tile_of(s.xf, layer, t, start) - tile_of(s.xf, layer, t, start - 1))
                flows = flows + (across_y[t][2] - yf[t]) + (tile_of(s.zf, layer + 1, t, start) - tile_of(s.zf, layer, t, start))
                s.q[layer, t, rows, :] = (tile_of(s.s0, layer, t, start) - stored) - ocean * p[t] - flows
        return carry

    lax.fori_loop(0, layers, one_layer, 0)


def product_tile(layers, s, v_ref, layer, start, count):
    v = tiles_of(v_ref, layer, start)
    north, south = from_north(v), from_south(v)
    upper = jnp.minimum(layer + 1, layers - 1)
    lower = jnp.maximum(layer - 1, 0)
    out = []
    for t in range(count):
        value = tile_of(s.c, layer, t, start) * v[t]
        value = value + (tile_of(s.xb, layer, t, start) * tile_of(v_ref, layer, t, start + 1)
                         - tile_of(s.xa, layer, t, start - 1) * tile_of(v_ref, layer, t, start - 1))
        value = value + (tile_of(s.yb, layer, t, start) * north[t] - tile_of(s.ya, layer, t, start) * south[t])
        value = value + (tile_of(s.zb, layer + 1, t, start) * tile_of(v_ref, upper, t, start)
                         - tile_of(s.za, layer, t, start) * tile_of(v_ref, lower, t, start))
        out.append(value)
    return v, out


def first_product(layers, starts, s):
    def one_layer(layer, carry):
        for start in starts:
            _, out = product_tile(layers, s, s.q, layer, start, NT)
            for t in range(NT):
                s.w[layer, t, pl.ds(start, 8), :] = out[t]
        return carry

    lax.fori_loop(0, layers, one_layer, 0)


def second_product(layers, starts, s, sums, z_ref):
    def one_layer(layer, sums):
        sums = list(sums)
        for start in starts:
            w, z = product_tile(layers, s, s.w, layer, start, NT - 1)
            for t in range(NT - 1):
                q = tile_of(s.q, layer, t, start)
                if z_ref is not None:
                    z_ref[layer, t, pl.ds(start - TOP, 8), :] = z[t]
                for i, (a, b) in enumerate(((q, q), (q, w[t]), (q, z[t]), (w[t], w[t]), (w[t], z[t]), (z[t], z[t]))):
                    sums[i] = sums[i] + a * b
        return tuple(sums)

    return lax.fori_loop(0, layers, one_layer, sums)


def put_sums(sums, out_ref):
    lane = lax.broadcasted_iota(jnp.int32, (1, 128), 1)
    row = jnp.zeros((1, 128), F32)
    for i, part in enumerate(sums):
        total = jnp.sum(jnp.sum(part, axis=0, keepdims=True), axis=1, keepdims=True)
        row = row + jnp.where(lane == i, total, 0.0)
    out_ref[...] = jnp.broadcast_to(row, out_ref.shape)


def step_weights(sums_ref):
    total = jnp.sum(sums_ref[...], axis=0, keepdims=True)
    lane = lax.broadcasted_iota(jnp.int32, (1, 128), 1)
    qq, qw, qz, ww, wz, zz = (
        jnp.sum(jnp.where(lane == i, total, 0.0), axis=1, keepdims=True) for i in range(6))
    first = qq + EPS
    qq, qw, qz, ww, wz, zz = (entry / first for entry in (qq, qw, qz, ww, wz, zz))
    norm = jnp.sqrt(first)
    h11 = qw
    left = jnp.maximum(ww - 2.0 * h11 * qw + h11 * h11 * qq, 0.0)
    square = left + EPS
    h21 = jnp.sqrt(square)
    h12 = (qz - h11 * qw) / h21
    h22 = (wz - h11 * qz - h11 * (ww - h11 * qw)) / square
    length = (zz - 2.0 * h11 * wz + h11 * h11 * ww) / square
    cross = (qw - h11 * qq) / h21
    rest = (length - 2.0 * (h12 * h12 + h22 * h22) + h12 * h12 * qq + h22 * h22 * (left / square)
            + 2.0 * h12 * h22 * cross)
    third = jnp.maximum(rest, 0.0) + EPS
    radius = jnp.sqrt(h11 * h11 + square)
    cosine = h11 / radius
    sine = h21 / radius
    top = cosine * h12 + sine * h22
    lower = cosine * h22 - sine * h12
    y2 = -lower * sine * norm / (lower * lower + third)
    y1 = (cosine * norm - top * y2) / radius
    b = y2 / (norm * h21)
    a = y1 / norm - b * h11
    return jnp.broadcast_to(a, (8, 128)), jnp.broadcast_to(b, (8, 128))


class Refs:
    def __init__(self, **refs):
        self.__dict__.update(refs)


COEFS = ("sig", "m", "s", "c", "xa", "xb", "ya", "yb", "za", "zb", "zf", "xf")


def coef_scratch(layers):
    return [pltpu.VMEM((layers + (name in ("za", "zb", "zf")), NT, ROWS, 128), F32) for name in COEFS]


def clear_bottom(s):
    zero = jnp.zeros((8, 128), F32)
    for ref in (s.za, s.zb, s.zf):
        for t in range(NT):
            for row in range(0, ROWS, 8):
                ref[0, t, row:row + 8, :] = zero


def first_kernel(layers, par_x, p_old, k_old, o_old, r_old, rech_old, act_old, got_a, got_b,
                 p_ref, k_ref, s0_ref, ap_ref, rech_ref, act_ref, tx, ty, tz, q_ref, w_ref, sums_ref,
                 ax, ay, *coefs):
    place_strips(layers, par_x[0] == 1, (p_ref, k_ref, s0_ref, ap_ref, rech_ref, act_ref), got_a, got_b)
    s = Refs(p=p_ref, k=k_ref, s0=s0_ref, ap=ap_ref, act=act_ref, tx=tx, ty=ty, tz=tz, q=q_ref, w=w_ref,
             ax=ax, ay=ay, **dict(zip(COEFS, coefs)))
    clear_bottom(s)
    def pairs(i, carry):
        start = 4 * i
        act = flat_tiles(act_ref, start)
        north = from_north(act)
        for t in range(NT):
            ax[t, pl.ds(start, 8), :] = 0.5 * act[t] * act_ref[t, pl.ds(start + 1, 8), :]
            ay[t, pl.ds(start, 8), :] = 0.5 * act[t] * north[t]
        return carry

    lax.fori_loop(0, 18, pairs, 0)

    def point(layer, carry):
        top = jnp.where(layer == layers - 1, 1.0, 0.0).astype(F32)
        for start in range(0, ROWS, 8):
            rows = pl.ds(start, 8)
            for t in range(NT):
                sigmoid_tile(tile_of(p_ref, layer, t, start), layer, t, start, s.sig, s.m, s.s)
                act = act_ref[t, rows, :]
                ap = (0.9 * act) * tile_of(ap_ref, layer, t, start)
                ap_ref[layer, t, rows, :] = ap
                s0_ref[layer, t, rows, :] = (
                    ap * jax.nn.sigmoid(tile_of(s0_ref, layer, t, start)) + (top * act) * rech_ref[t, rows, :])
        return carry

    lax.fori_loop(0, layers, point, 0)
    starts = range(4, 76, 8)
    far_faces(layers, (0, *starts), s, True)
    assemble(layers, starts, s, True)
    first_product(layers, starts, s)
    sums = tuple(jnp.zeros((8, 128), F32) for _ in range(6))
    sums = second_product(layers, range(TOP, TOP + 64, 8), s, sums, None)
    put_sums(sums, sums_ref)


def next_kernel(layers, p_old, s0_ref, ap_ref, act_ref, tx, ty, tz, q_old, w_old, got_ref,
                p_ref, q_ref, w_ref, z_ref, sums_ref, *coefs):
    a, b = step_weights(got_ref)
    s = Refs(p=p_ref, s0=s0_ref, ap=ap_ref, act=act_ref, tx=tx, ty=ty, tz=tz, q=q_ref, w=w_ref,
             **dict(zip(COEFS, coefs)))
    clear_bottom(s)

    def point(layer, carry):
        for start in range(4, 76, 8):
            rows = pl.ds(start, 8)
            for t in range(NT):
                p = tile_of(p_ref, layer, t, start) + (
                    a * tile_of(q_ref, layer, t, start) + b * tile_of(w_ref, layer, t, start))
                p_ref[layer, t, rows, :] = p
                sigmoid_tile(p, layer, t, start, s.sig, s.m, s.s)
        return carry

    lax.fori_loop(0, layers, point, 0)
    starts = range(4, 76, 8)
    far_faces(layers, (0, *starts), s, False)
    assemble(layers, starts, s, False)
    first_product(layers, starts, s)
    sums = tuple(jnp.zeros((8, 128), F32) for _ in range(6))
    sums = second_product(layers, range(TOP, TOP + 64, 8), s, sums, z_ref)
    put_sums(sums, sums_ref)


def last_kernel(layers, p_ref, q_ref, w_ref, z_ref, got_ref, final_out, left_out, final_buf, left_buf, sems):
    a, b = step_weights(got_ref)
    for layer in range(layers):
        for start in range(0, 64, 8):
            for t in range(NT - 1):
                q = q_ref[layer, t, TOP + start:TOP + start + 8, :]
                w = w_ref[layer, t, TOP + start:TOP + start + 8, :]
                place = (layer, slice(start, start + 8), slice(128 * t, 128 * t + 128))
                final_buf[place] = p_ref[layer, t, TOP + start:TOP + start + 8, :] + (a * q + b * w)
                left_buf[place] = (q - a * w) - b * z_ref[layer, t, start:start + 8, :]
        pltpu.make_async_copy(final_buf.at[layer], final_out.at[layer], sems.at[layer, 0]).start()
        pltpu.make_async_copy(left_buf.at[layer], left_out.at[layer], sems.at[layer, 1]).start()
    for layer in range(layers):
        pltpu.make_async_copy(final_buf.at[layer], final_out.at[layer], sems.at[layer, 0]).wait()
        pltpu.make_async_copy(left_buf.at[layer], left_out.at[layer], sems.at[layer, 1]).wait()


VM = pl.BlockSpec(memory_space=pltpu.VMEM)
HB = pl.BlockSpec(memory_space=pl.ANY)
SM = pl.BlockSpec(memory_space=pltpu.SMEM)


def grant(mib):
    return pltpu.CompilerParams(vmem_limit_bytes=mib * 1024 * 1024)


def keep(*arrays):
    return [pltpu.with_memory_space_constraint(array, pltpu.VMEM) for array in arrays]


def outside(*arrays):
    return [pltpu.with_memory_space_constraint(array, pltpu.HBM) for array in arrays]


def swap(value, axes, first):
    size = lax.axis_size(axes)
    pairs = [(i, i + 1) for i in range(first, size - 1, 2)]
    return lax.ppermute(value, axes, pairs + [(b, a) for a, b in pairs])


def bound(kernel, *args):
    def call(*refs):
        kernel(*args, *refs)

    return call


def body(pressure, pressure_old, conductivity, porosity, recharge, active):
    layers = pressure.shape[0]
    par_x = (lax.axis_index(GX) % 2).astype(jnp.int32).reshape(1)
    par_y = (lax.axis_index(GY) % 2).astype(jnp.int32).reshape(1)
    field = pltpu.VMEM((layers, NT, ROWS, 128), F32)
    plane = pltpu.VMEM((NT, ROWS, 128), F32)
    strip_y = pltpu.VMEM((2, 64, 128), F32)
    strip_x = pltpu.VMEM((NT, 192, 128), F32)
    state = (field,) * 4 + (plane,) * 2
    *fields, send_a, send_b = pl.pallas_call(
        bound(load_kernel, layers), name="load", out_shape=state + (strip_y,) * 2,
        in_specs=[SM] + [HB] * 6, out_specs=(VM,) * 8,
        scratch_shapes=[pltpu.VMEM((4, 64, 128), jnp.int32), pltpu.SemaphoreType.DMA((24,))],
        compiler_params=grant(6),
    )(par_y, *outside(pressure, conductivity, pressure_old, porosity, recharge, active))
    got_a = swap(send_a, GY, 0)
    got_b = swap(send_b, GY, 1)
    *fields, send_a, send_b = pl.pallas_call(
        bound(turn_kernel, layers), name="turn", out_shape=state + (strip_x,) * 2,
        in_specs=[SM] * 2 + [VM] * 8, out_specs=(VM,) * 8,
        input_output_aliases={i + 2: i for i in range(6)}, compiler_params=grant(6),
    )(par_y, par_x, *keep(*fields), got_a, got_b)
    got_a = swap(send_a, GX, 0)
    got_b = swap(send_b, GX, 1)
    p, _, s0, ap, _, act, tx, ty, tz, q, w, sums = pl.pallas_call(
        bound(first_kernel, layers), name="first",
        out_shape=state + (field,) * 5 + (jax.ShapeDtypeStruct((128, 128), F32),),
        in_specs=[SM] + [VM] * 8, out_specs=(VM,) * 12,
        input_output_aliases={i + 1: i for i in range(6)},
        scratch_shapes=[plane, plane] + coef_scratch(layers), compiler_params=grant(30),
    )(par_x, *keep(*fields), got_a, got_b)
    sums = lax.all_to_all(sums, ALL, 0, 0, tiled=True)
    p, q, w, z, sums = pl.pallas_call(
        bound(next_kernel, layers), name="next",
        out_shape=(field,) * 3 + (pltpu.VMEM((layers, 4, 64, 128), F32), jax.ShapeDtypeStruct((128, 128), F32)),
        in_specs=[VM] * 10, out_specs=(VM,) * 5, input_output_aliases={0: 0, 7: 1, 8: 2},
        scratch_shapes=coef_scratch(layers), compiler_params=grant(30),
    )(*keep(p, s0, ap, act, tx, ty, tz, q, w), sums)
    sums = lax.all_to_all(sums, ALL, 0, 0, tiled=True)
    out = jax.ShapeDtypeStruct(pressure.shape, F32)
    block = pltpu.VMEM(pressure.shape, F32)
    return pl.pallas_call(
        bound(last_kernel, layers), name="last", out_shape=(out, out),
        in_specs=[VM] * 5, out_specs=(HB, HB),
        scratch_shapes=[block, block, pltpu.SemaphoreType.DMA((layers, 2))], compiler_params=grant(8),
    )(*keep(p, q, w, z), sums)


def solution(mesh):
    torus = Mesh(mesh.devices.reshape(4, 4, 4, 2), ALL)
    field = P(None, GX, GY)
    plane = P(GX, GY)
    return jax.shard_map(
        body, mesh=torus, in_specs=(field,) * 4 + (plane,) * 2, out_specs=(field, field), check_vma=False)
```

```python
import jax
import jax.numpy as jnp
from jax import lax
from jax.experimental import pallas as pl
from jax.experimental.pallas import tpu as pltpu
from jax.sharding import Mesh
from jax.sharding import PartitionSpec as P

GX = ("gx_0", "gx_1")
GY = ("gy_0", "gy_1")
ALL = GX + GY

EPS = 1e-06
NT = 5
ROWS = 80
TOP = 8
SPAN = 416
F32 = jnp.float32


def lanes():
    return lax.broadcasted_iota(jnp.int32, (8, 128), 1)


def from_north(tiles):
    lane = lanes()
    turned = [pltpu.roll(tile, 127, 1) for tile in tiles]
    count = len(tiles)
    return [jnp.where(lane == 127, turned[(t + 1) % count], turned[t]) for t in range(count)]


def from_south(tiles):
    lane = lanes()
    turned = [pltpu.roll(tile, 1, 1) for tile in tiles]
    count = len(tiles)
    return [jnp.where(lane == 0, turned[(t - 1) % count], turned[t]) for t in range(count)]


def at(t, start, size=8):
    return pl.ds(ROWS * t + start, size)


def tile_of(ref, layer, t, start):
    return ref[layer, at(t, start), :]


def tiles_of(ref, layer, start):
    return [tile_of(ref, layer, t, start) for t in range(NT)]


def flat_tiles(ref, start):
    return [ref[at(t, start), :] for t in range(NT)]


UNITS = 25


def strip_units(layers):
    return [(f, layer) for f in range(4) for layer in range(layers)] + [(4, None), (5, None)]


def edge_kernel(layers, par, p_in, k_in, o_in, r_in, act_in, rech_in, send_a, send_b, edges, act_edges, rech_edges, sems):
    copies = []
    for side, first in ((0, 0), (1, 384)):
        cols = pl.ds(first, 128)
        for f, src in enumerate((p_in, k_in, o_in, r_in)):
            copies.append(pltpu.make_async_copy(src.at[:, :, cols], edges.at[f, side], sems.at[side * 6 + f]))
        copies.append(pltpu.make_async_copy(act_in.at[:, cols], act_edges.at[side], sems.at[side * 6 + 4]))
        copies.append(pltpu.make_async_copy(rech_in.at[:, cols], rech_edges.at[side], sems.at[side * 6 + 5]))
    for copy in copies:
        copy.start()
    for copy in copies:
        copy.wait()
    first = lanes() < 5
    last = lanes() >= 123
    odd = par[0] == 1
    zero = jnp.zeros((8, 128), F32)

    def pack(row, carry):
        rows = pl.ds(pl.multiple_of(8 * row, 8), 8)
        low = [zero, zero]
        high = [zero, zero]
        for u, (f, layer) in enumerate(strip_units(layers)):
            place = 5 * (u % UNITS)
            here = u // UNITS
            if f == 4:
                a, b = act_edges[0, rows, :].astype(F32), act_edges[1, rows, :].astype(F32)
            elif f == 5:
                a, b = rech_edges[0, rows, :], rech_edges[1, rows, :]
            else:
                a, b = edges[f, 0, layer, rows, :], edges[f, 1, layer, rows, :]
            a = jnp.where(first, a, 0.0)
            b = jnp.where(last, b, 0.0)
            low[here] = low[here] + (pltpu.roll(a, place, 1) if place else a)
            high[here] = high[here] + pltpu.roll(b, (place + 5) % 128, 1)
        for here in range(2):
            send_a[here, rows, :] = jnp.where(odd, low[here], high[here])
            send_b[here, rows, :] = jnp.where(odd, high[here], low[here])
        return carry

    lax.fori_loop(0, 8, pack, 0)


def unpack_strips(layers, odd, got_a, got_b, rows, put):
    left_edge = lanes() >= 123
    right_edge = lanes() < 5
    a = [got_a[here, rows, :] for here in range(2)]
    b = [got_b[here, rows, :] for here in range(2)]
    below = [jnp.where(odd, a[h], b[h]) for h in range(2)]
    above = [jnp.where(odd, b[h], a[h]) for h in range(2)]
    for u, (f, layer) in enumerate(strip_units(layers)):
        place = 5 * (u % UNITS)
        here = u // UNITS
        left = pltpu.roll(below[here], (123 - place) % 128, 1)
        right = pltpu.roll(above[here], 128 - place, 1) if place else above[here]
        put(f, layer, jnp.where(left_edge, left, jnp.where(right_edge, right, 0.0)))


STRIP_ROWS = ((0, 5), (5, 5), (10, 4), (14, 4))


def turn_kernel(layers, par_y, par_x, p_in, k_in, o_in, r_in, act_in, rech_in, got_a, got_b,
                send_a, send_b, edges, act_edges, rech_edges, act_int, sems):
    copies = []
    for side, first in ((0, 0), (1, 56)):
        rows = pl.ds(first, 8)
        for t in range(4):
            cols = pl.ds(128 * t, 128)
            for f, src in enumerate((p_in, k_in, o_in, r_in)):
                copies.append(pltpu.make_async_copy(
                    src.at[:, rows, cols], edges.at[f, side, :, t], sems.at[side, t, f]))
            copies.append(pltpu.make_async_copy(act_in.at[rows, cols], act_int.at[side, t], sems.at[side, t, 4]))
            copies.append(pltpu.make_async_copy(rech_in.at[rows, cols], rech_edges.at[side, t], sems.at[side, t, 5]))
    for copy in copies:
        copy.start()
    odd = par_y[0] == 1
    for side in range(2):
        def put(f, layer, value):
            if f == 4:
                act_edges[side, 4] = value
            elif f == 5:
                rech_edges[side, 4] = value
            else:
                edges[f, side, layer, 4] = value

        unpack_strips(layers, odd, got_a, got_b, pl.ds(56 * side, 8), put)
    for copy in copies:
        copy.wait()
    for side in range(2):
        for t in range(4):
            act_edges[side, t] = act_int[side, t].astype(F32)
    for send, side in ((send_a, 1 - par_x[0]), (send_b, par_x[0])):
        start5 = 3 * side
        start4 = 4 * side

        def fill(layer, carry):
            for f, (place, depth) in enumerate(STRIP_ROWS):
                start = start5 if depth == 5 else start4
                for t in range(NT):
                    send[t, pl.ds(layer * 18 + place, depth), :] = edges[f, side, layer, t, pl.ds(start, depth), :]
            return carry

        lax.fori_loop(0, layers, fill, 0)
        for t in range(NT):
            send[t, 18 * layers:18 * layers + 5, :] = act_edges[side, t, pl.ds(start5, 5), :]
            send[t, 18 * layers + 5:18 * layers + 9, :] = rech_edges[side, t, pl.ds(start4, 4), :]


def place_strips(layers, up, refs, got_a, got_b):
    p_ref, k_ref, o_ref, r_ref, rech_ref, act_ref = refs
    fields = (p_ref, k_ref, o_ref, r_ref)
    low, high = TOP, TOP + 64
    for got, above in ((got_a, jnp.logical_not(up)), (got_b, up)):
        dst5 = jnp.where(above, high, low - 5)
        dst4 = jnp.where(above, high, low - 4)

        def fill(layer, carry):
            for (place, depth), ref in zip(STRIP_ROWS, fields):
                start = dst5 if depth == 5 else dst4
                for t in range(NT):
                    ref[layer, at(t, start, depth), :] = got[t, pl.ds(layer * 18 + place, depth), :]
            return carry

        lax.fori_loop(0, layers, fill, 0)
        for t in range(NT):
            act_ref[at(t, dst5, 5), :] = got[t, 18 * layers:18 * layers + 5, :]
            rech_ref[at(t, dst4, 4), :] = got[t, 18 * layers + 5:18 * layers + 9, :]


def sigmoid_tile(value, layer, t, start, sig_ref, mob_ref, der_ref):
    sig = jax.nn.sigmoid(value)
    square = sig * sig
    sig_ref[layer, at(t, start), :] = sig
    mob_ref[layer, at(t, start), :] = 0.5 * square
    der_ref[layer, at(t, start), :] = square - square * sig


def face(trans, p_a, p_b, m_a, m_b, s_a, s_b, gravity):
    drop = p_a - p_b
    if gravity:
        drop = drop + gravity
    by_mob = trans * (m_a + m_b)
    by_drop = trans * drop
    return by_mob + s_a * by_drop, s_b * by_drop - by_mob, by_mob * drop


def far_faces(layers, starts, s, make_trans):
    def one_layer(layer, carry):
        upper = jnp.minimum(layer + 1, layers - 1)
        inner = jnp.where(layer + 1 < layers, 1.0, 0.0).astype(F32)
        for start in starts:
            for t in range(NT):
                here = at(t, start)
                if make_trans:
                    trans = s.ax[here, :] * (tile_of(s.k, layer, t, start) + tile_of(s.k, layer, t, start + 1))
                    s.tx[layer, here, :] = trans
                else:
                    trans = tile_of(s.tx, layer, t, start)
                p = tile_of(s.p, layer, t, start)
                m = tile_of(s.m, layer, t, start)
                der = tile_of(s.s, layer, t, start)
                ca, cb, flow = face(
                    trans, p, tile_of(s.p, layer, t, start + 1), m, tile_of(s.m, layer, t, start + 1),
                    der, tile_of(s.s, layer, t, start + 1), 0.0)
                s.xa[layer, here, :] = ca
                s.xb[layer, here, :] = cb
                s.xf[layer, here, :] = flow
                if make_trans:
                    trans = (s.act[here, :] * inner) * (
                        tile_of(s.k, layer, t, start) + tile_of(s.k, upper, t, start))
                    s.tz[layer, here, :] = trans
                else:
                    trans = tile_of(s.tz, layer, t, start)
                za, zb, zf = face(
                    trans, p, tile_of(s.p, upper, t, start), m, tile_of(s.m, upper, t, start),
                    der, tile_of(s.s, upper, t, start), -1.0)
                s.za[layer + 1, here, :] = za
                s.zb[layer + 1, here, :] = zb
                s.zf[layer + 1, here, :] = zf
        return carry

    lax.fori_loop(0, layers, one_layer, 0)


def assemble(layers, starts, s, make_trans):
    def one_layer(layer, carry):
        for start in starts:
            p = tiles_of(s.p, layer, start)
            m = tiles_of(s.m, layer, start)
            der = tiles_of(s.s, layer, start)
            if make_trans:
                k = tiles_of(s.k, layer, start)
                k_north = from_north(k)
                ty = [s.ay[at(t, start), :] * (k[t] + k_north[t]) for t in range(NT)]
                for t in range(NT):
                    s.ty[layer, at(t, start), :] = ty[t]
            else:
                ty = tiles_of(s.ty, layer, start)
            p_north, m_north, s_north = from_north(p), from_north(m), from_north(der)
            across_y = [face(ty[t], p[t], p_north[t], m[t], m_north[t], der[t], s_north[t], 0.0) for t in range(NT)]
            ya = from_south([f[0] for f in across_y])
            yb = from_south([f[1] for f in across_y])
            yf = from_south([f[2] for f in across_y])
            for t in range(NT):
                here = at(t, start)
                s.ya[layer, here, :] = ya[t]
                s.yb[layer, here, :] = across_y[t][1]
                sig = tile_of(s.sig, layer, t, start)
                ap = tile_of(s.ap, layer, t, start)
                ocean = 1.0 - s.act[here, :]
                stored = ap * sig
                center = (stored - stored * sig) + ocean
                center = center + (tile_of(s.xa, layer, t, start) - tile_of(s.xb, layer, t, start - 1))
                center = center + (across_y[t][0] - yb[t]) + (tile_of(s.za, layer + 1, t, start) - tile_of(s.zb, layer, t, start))
                s.c[layer, here, :] = center
                flows = (tile_of(s.xf, layer, t, start) - tile_of(s.xf, layer, t, start - 1))
                flows = flows + (across_y[t][2] - yf[t]) + (tile_of(s.zf, layer + 1, t, start) - tile_of(s.zf, layer, t, start))
                s.q[layer, here, :] = (tile_of(s.s0, layer, t, start) - stored) - ocean * p[t] - flows
        return carry

    lax.fori_loop(0, layers, one_layer, 0)


def product_tile(layers, s, v_ref, layer, start, count):
    v = tiles_of(v_ref, layer, start)
    north, south = from_north(v), from_south(v)
    upper = jnp.minimum(layer + 1, layers - 1)
    lower = jnp.maximum(layer - 1, 0)
    out = []
    for t in range(count):
        value = tile_of(s.c, layer, t, start) * v[t]
        value = value + (tile_of(s.xb, layer, t, start) * tile_of(v_ref, layer, t, start + 1)
                         - tile_of(s.xa, layer, t, start - 1) * tile_of(v_ref, layer, t, start - 1))
        value = value + (tile_of(s.yb, layer, t, start) * north[t] - tile_of(s.ya, layer, t, start) * south[t])
        value = value + (tile_of(s.zb, layer + 1, t, start) * tile_of(v_ref, upper, t, start)
                         - tile_of(s.za, layer, t, start) * tile_of(v_ref, lower, t, start))
        out.append(value)
    return v, out


def first_product(layers, starts, s):
    def one_layer(layer, carry):
        for start in starts:
            _, out = product_tile(layers, s, s.q, layer, start, NT)
            for t in range(NT):
                s.w[layer, at(t, start), :] = out[t]
        return carry

    lax.fori_loop(0, layers, one_layer, 0)


def second_product(layers, starts, s, sums, z_ref):
    def one_layer(layer, sums):
        sums = list(sums)
        for start in starts:
            w, z = product_tile(layers, s, s.w, layer, start, NT - 1)
            for t in range(NT - 1):
                q = tile_of(s.q, layer, t, start)
                if z_ref is not None:
                    z_ref[layer, pl.ds(64 * t + start - TOP, 8), :] = z[t]
                for i, (a, b) in enumerate(((q, q), (q, w[t]), (q, z[t]), (w[t], w[t]), (w[t], z[t]), (z[t], z[t]))):
                    sums[i] = sums[i] + a * b
        return tuple(sums)

    return lax.fori_loop(0, layers, one_layer, sums)


def put_sums(sums, out_ref):
    lane = lax.broadcasted_iota(jnp.int32, (1, 128), 1)
    row = jnp.zeros((1, 128), F32)
    for i, part in enumerate(sums):
        total = jnp.sum(jnp.sum(part, axis=0, keepdims=True), axis=1, keepdims=True)
        row = row + jnp.where(lane == i, total, 0.0)
    out_ref[...] = jnp.broadcast_to(row, out_ref.shape)


def step_weights(sums_ref):
    total = jnp.sum(sums_ref[...], axis=0, keepdims=True)
    lane = lax.broadcasted_iota(jnp.int32, (1, 128), 1)
    qq, qw, qz, ww, wz, zz = (
        jnp.sum(jnp.where(lane == i, total, 0.0), axis=1, keepdims=True) for i in range(6))
    first = qq + EPS
    qq, qw, qz, ww, wz, zz = (entry / first for entry in (qq, qw, qz, ww, wz, zz))
    norm = jnp.sqrt(first)
    h11 = qw
    left = jnp.maximum(ww - 2.0 * h11 * qw + h11 * h11 * qq, 0.0)
    square = left + EPS
    h21 = jnp.sqrt(square)
    h12 = (qz - h11 * qw) / h21
    h22 = (wz - h11 * qz - h11 * (ww - h11 * qw)) / square
    length = (zz - 2.0 * h11 * wz + h11 * h11 * ww) / square
    cross = (qw - h11 * qq) / h21
    rest = (length - 2.0 * (h12 * h12 + h22 * h22) + h12 * h12 * qq + h22 * h22 * (left / square)
            + 2.0 * h12 * h22 * cross)
    third = jnp.maximum(rest, 0.0) + EPS
    radius = jnp.sqrt(h11 * h11 + square)
    cosine = h11 / radius
    sine = h21 / radius
    top = cosine * h12 + sine * h22
    lower = cosine * h22 - sine * h12
    y2 = -lower * sine * norm / (lower * lower + third)
    y1 = (cosine * norm - top * y2) / radius
    b = y2 / (norm * h21)
    a = y1 / norm - b * h11
    return jnp.broadcast_to(a, (8, 128)), jnp.broadcast_to(b, (8, 128))


class Refs:
    def __init__(self, **refs):
        self.__dict__.update(refs)


STATE = ("p", "k", "s0", "ap", "tx", "ty", "tz", "q", "w")
COEFS = ("c", "xa", "xb", "ya", "yb", "za", "zb", "xf", "zf")
POINT = ("sig", "m", "s")
TALL = ("za", "zb", "zf")


def space(layers, name):
    return pltpu.VMEM((layers + (name in TALL), SPAN, 128), F32)


def clear_bottom(s):
    zero = jnp.zeros((8, 128), F32)

    def clear(i, carry):
        for ref in (s.za, s.zb, s.zf):
            ref[0, pl.ds(pl.multiple_of(8 * i, 8), 8), :] = zero
        return carry

    lax.fori_loop(0, SPAN // 8, clear, 0)


def mask_pairs(s, starts):
    for start in starts:
        act = flat_tiles(s.act, start)
        north = from_north(act)
        for t in range(NT):
            s.ax[at(t, start), :] = 0.5 * act[t] * s.act[at(t, start + 1), :]
            s.ay[at(t, start), :] = 0.5 * act[t] * north[t]


def points(layers, s, new, old):
    def point(layer, carry):
        top = jnp.where(layer == layers - 1, 1.0, 0.0).astype(F32)
        for start in (*new, *old):
            for t in range(NT):
                sigmoid_tile(tile_of(s.p, layer, t, start), layer, t, start, s.sig, s.m, s.s)
                if start in new:
                    act = s.act[at(t, start), :]
                    ap = (0.9 * act) * tile_of(s.ap, layer, t, start)
                    s.ap[layer, at(t, start), :] = ap
                    s.s0[layer, at(t, start), :] = (
                        ap * jax.nn.sigmoid(tile_of(s.s0, layer, t, start)) + (top * act) * s.rech[at(t, start), :])
        return carry

    lax.fori_loop(0, layers, point, 0)


def inner_kernel(layers, par_y, p_in, k_in, o_in, r_in, act_in, rech_in, got_a, got_b, after, *refs):
    names = STATE + COEFS + ("act", "rech", "ax", "ay")
    s = Refs(**dict(zip(names, refs)))
    part_ref = refs[len(names)]
    s.sig, s.m, s.s, act_int, sems = refs[len(names) + 1:]
    copies = []
    for t in range(4):
        cols = pl.ds(128 * t, 128)
        for f, (src, dst) in enumerate(((p_in, s.p), (k_in, s.k), (o_in, s.s0), (r_in, s.ap))):
            copies.append(pltpu.make_async_copy(src.at[:, :, cols], dst.at[:, at(t, TOP, 64), :], sems.at[t, f]))
        copies.append(pltpu.make_async_copy(act_in.at[:, cols], act_int.at[t], sems.at[t, 4]))
        copies.append(pltpu.make_async_copy(rech_in.at[:, cols], s.rech.at[at(t, TOP, 64), :], sems.at[t, 5]))
    for copy in copies:
        copy.start()
    zero = jnp.zeros((8, 128), F32)
    fields = (s.p, s.k, s.s0, s.ap)

    def clear(layer, carry):
        for ref in fields:
            for t in range(NT):
                ref[layer, at(t, 0), :] = zero
                ref[layer, at(t, ROWS - 8), :] = zero
        return carry

    lax.fori_loop(0, layers, clear, 0)
    for ref in (s.act, s.rech):
        for t in range(NT):
            ref[at(t, 0), :] = zero
            ref[at(t, ROWS - 8), :] = zero
    clear_bottom(s)
    odd = par_y[0] == 1

    def unpack(row, carry):
        start = pl.multiple_of(TOP + 8 * row, 8)

        def put(f, layer, value):
            if f == 4:
                s.act[at(4, start), :] = value
            elif f == 5:
                s.rech[at(4, start), :] = value
            else:
                fields[f][layer, at(4, start), :] = value

        unpack_strips(layers, odd, got_a, got_b, pl.ds(pl.multiple_of(8 * row, 8), 8), put)
        return carry

    lax.fori_loop(0, 8, unpack, 0)
    for copy in copies:
        copy.wait()
    for t in range(4):
        s.act[at(t, TOP, 64), :] = act_int[t].astype(F32)
    points(layers, s, range(8, 72, 8), ())
    mask_pairs(s, (*range(8, 64, 8), 63))
    far_faces(layers, (*range(8, 64, 8), 63), s, True)
    assemble(layers, range(12, 68, 8), s, True)
    first_product(layers, range(20, 60, 8), s)
    sums = second_product(layers, range(24, 56, 8), s, (zero,) * 6, None)
    for i in range(6):
        part_ref[i] = sums[i]


def first_kernel(layers, par_x, *refs):
    names = STATE + COEFS + ("act", "rech", "ax", "ay")
    count = len(names)
    part_ref, got_a, got_b = refs[count:count + 3]
    refs = refs[count + 3:]
    s = Refs(**dict(zip(names, refs)))
    sums_ref = refs[count]
    s.sig, s.m, s.s = refs[count + 1:]
    place_strips(layers, par_x[0] == 1, (s.p, s.k, s.s0, s.ap, s.rech, s.act), got_a, got_b)
    points(layers, s, (0, 72), (8, 64))
    mask_pairs(s, (0, 4, 64, 68))
    far_faces(layers, (0, 64, 68), s, True)
    assemble(layers, (4, 68), s, True)
    first_product(layers, (4, 12, 60, 68), s)
    sums = second_product(layers, (8, 16, 56, 64), s, tuple(part_ref[i] for i in range(6)), None)
    put_sums(sums, sums_ref)


KEPT = ("s0", "ap", "tx", "ty", "tz", "act")
SHARED = 4
MOVED = ("p", "q", "w") + COEFS[:SHARED]


def next_kernel(layers, *refs):
    kept, refs = refs[:len(KEPT)], refs[len(KEPT) + len(MOVED):]
    got_ref, *refs = refs
    s = Refs(**dict(zip(KEPT, kept)), **dict(zip(MOVED, refs)))
    z_ref, sums_ref, *own = refs[len(MOVED):]
    for name, ref in zip(COEFS[SHARED:] + POINT, own):
        setattr(s, name, ref)
    p_ref, q_ref, w_ref = s.p, s.q, s.w
    a, b = step_weights(got_ref)
    if SHARED < len(COEFS):
        clear_bottom(s)

    def point(layer, carry):
        for start in range(4, 76, 8):
            for t in range(NT):
                p = tile_of(p_ref, layer, t, start) + (
                    a * tile_of(q_ref, layer, t, start) + b * tile_of(w_ref, layer, t, start))
                p_ref[layer, at(t, start), :] = p
                sigmoid_tile(p, layer, t, start, s.sig, s.m, s.s)
        return carry

    lax.fori_loop(0, layers, point, 0)
    starts = range(4, 76, 8)
    far_faces(layers, (0, *starts), s, False)
    assemble(layers, starts, s, False)
    first_product(layers, starts, s)
    sums = tuple(jnp.zeros((8, 128), F32) for _ in range(6))
    sums = second_product(layers, range(TOP, TOP + 64, 8), s, sums, z_ref)
    put_sums(sums, sums_ref)


def last_kernel(layers, p_ref, q_ref, w_ref, z_ref, got_ref, final_out, left_out, final_buf, left_buf, sems):
    a, b = step_weights(got_ref)
    for layer in range(layers):
        for start in range(0, 64, 8):
            for t in range(NT - 1):
                q = tile_of(q_ref, layer, t, TOP + start)
                w = tile_of(w_ref, layer, t, TOP + start)
                place = (layer, slice(start, start + 8), slice(128 * t, 128 * t + 128))
                final_buf[place] = tile_of(p_ref, layer, t, TOP + start) + (a * q + b * w)
                left_buf[place] = (q - a * w) - b * z_ref[layer, pl.ds(64 * t + start, 8), :]
        pltpu.make_async_copy(final_buf.at[layer], final_out.at[layer], sems.at[layer, 0]).start()
        pltpu.make_async_copy(left_buf.at[layer], left_out.at[layer], sems.at[layer, 1]).start()
    for layer in range(layers):
        pltpu.make_async_copy(final_buf.at[layer], final_out.at[layer], sems.at[layer, 0]).wait()
        pltpu.make_async_copy(left_buf.at[layer], left_out.at[layer], sems.at[layer, 1]).wait()


VM = pl.BlockSpec(memory_space=pltpu.VMEM)
HB = pl.BlockSpec(memory_space=pl.ANY)
SM = pl.BlockSpec(memory_space=pltpu.SMEM)


def grant(mib):
    return pltpu.CompilerParams(vmem_limit_bytes=mib * 1024 * 1024)


def keep(*arrays):
    return [pltpu.with_memory_space_constraint(array, pltpu.VMEM) for array in arrays]


def outside(*arrays):
    return [pltpu.with_memory_space_constraint(array, pltpu.HBM) for array in arrays]


def swap(value, axes, first):
    size = lax.axis_size(axes)
    pairs = [(i, i + 1) for i in range(first, size - 1, 2)]
    return lax.ppermute(value, axes, pairs + [(b, a) for a, b in pairs])


def bound(kernel, *args):
    def call(*refs):
        kernel(*args, *refs)

    return call


def body(pressure, pressure_old, conductivity, porosity, recharge, active):
    layers = pressure.shape[0]
    par_x = (lax.axis_index(GX) % 2).astype(jnp.int32).reshape(1)
    par_y = (lax.axis_index(GY) % 2).astype(jnp.int32).reshape(1)
    inputs = outside(pressure, conductivity, pressure_old, porosity, active, recharge)
    dma = pltpu.SemaphoreType.DMA
    strip_y = pltpu.VMEM((2, 64, 128), F32)
    strip_x = pltpu.VMEM((NT, 192, 128), F32)
    plane = pltpu.VMEM((SPAN, 128), F32)
    part = pltpu.VMEM((6, 8, 128), F32)
    block = jax.ShapeDtypeStruct((128, 128), F32)
    send_a, send_b = pl.pallas_call(
        bound(edge_kernel, layers), name="edge", out_shape=(strip_y,) * 2, in_specs=[SM] + [HB] * 6, out_specs=(VM,) * 2,
        scratch_shapes=[pltpu.VMEM((4, 2, layers, 64, 128), F32), pltpu.VMEM((2, 64, 128), jnp.int32),
                        pltpu.VMEM((2, 64, 128), F32), dma((12,))],
        compiler_params=grant(GRANT),
    )(par_y, *inputs)
    y_a = swap(send_a, GY, 0)
    y_b = swap(send_b, GY, 1)
    send_a, send_b = pl.pallas_call(
        bound(turn_kernel, layers), name="turn", out_shape=(strip_x,) * 2, in_specs=[SM] * 2 + [HB] * 6 + [VM] * 2,
        out_specs=(VM,) * 2,
        scratch_shapes=[pltpu.VMEM((4, 2, layers, NT, 8, 128), F32), pltpu.VMEM((2, NT, 8, 128), F32),
                        pltpu.VMEM((2, NT, 8, 128), F32), pltpu.VMEM((2, 4, 8, 128), jnp.int32), dma((2, 4, 6))],
        compiler_params=grant(GRANT),
    )(par_y, par_x, *inputs, y_a, y_b)
    x_a = swap(send_a, GX, 0)
    x_b = swap(send_b, GX, 1)
    state = tuple(space(layers, name) for name in STATE + COEFS) + (plane,) * 4
    points_scratch = [space(layers, name) for name in POINT]
    *fields, part_sums = pl.pallas_call(
        bound(inner_kernel, layers), name="inner", out_shape=state + (part,),
        in_specs=[SM] + [HB] * 6 + [VM] * 3, out_specs=(VM,) * (len(state) + 1),
        scratch_shapes=points_scratch + [pltpu.VMEM((4, 64, 128), jnp.int32), dma((4, 6))],
        compiler_params=grant(GRANT),
        cost_estimate=pl.CostEstimate(flops=100_000_000, transcendentals=0, bytes_accessed=6_000_000),
    )(par_y, *inputs, y_a, y_b, send_a)
    *fields, sums = pl.pallas_call(
        bound(first_kernel, layers), name="first", out_shape=state + (block,),
        in_specs=[SM] + [VM] * (len(state) + 3), out_specs=(VM,) * (len(state) + 1),
        input_output_aliases={i + 1: i for i in range(len(state))},
        scratch_shapes=points_scratch, compiler_params=grant(GRANT),
    )(par_x, *keep(*fields, part_sums), x_a, x_b)
    sums = lax.all_to_all(sums, ALL, 0, 0, tiled=True)
    named = dict(zip(STATE + COEFS + ("act", "rech", "ax", "ay"), fields))
    moved = tuple(space(layers, name) for name in MOVED)
    p, q, w, *rest = pl.pallas_call(
        bound(next_kernel, layers), name="next",
        out_shape=moved + (pltpu.VMEM((layers, 256, 128), F32), block),
        in_specs=[VM] * (len(KEPT) + len(MOVED) + 1), out_specs=(VM,) * (len(MOVED) + 2),
        input_output_aliases={len(KEPT) + i: i for i in range(len(MOVED))},
        scratch_shapes=[space(layers, name) for name in COEFS[SHARED:] + POINT], compiler_params=grant(GRANT2),
    )(*keep(*(named[n] for n in KEPT + MOVED)), sums)
    z, sums = rest[-2:]
    sums = lax.all_to_all(sums, ALL, 0, 0, tiled=True)
    out = jax.ShapeDtypeStruct(pressure.shape, F32)
    buffer = pltpu.VMEM(pressure.shape, F32)
    return pl.pallas_call(
        bound(last_kernel, layers), name="last", out_shape=(out, out), in_specs=[VM] * 5, out_specs=(HB, HB),
        scratch_shapes=[buffer, buffer, dma((layers, 2))], compiler_params=grant(GRANT),
    )(*keep(p, q, w, z), sums)


GRANT = 10
GRANT2 = 20


def solution(mesh):
    torus = Mesh(mesh.devices.reshape(4, 4, 4, 2), ALL)
    field = P(None, GX, GY)
    plane = P(GX, GY)
    return jax.shard_map(
        body, mesh=torus, in_specs=(field,) * 4 + (plane,) * 2, out_specs=(field, field), check_vma=False)
```

```python
import jax
import jax.numpy as jnp
from jax import lax
from jax.experimental import pallas as pl
from jax.experimental.pallas import tpu as pltpu
from jax.sharding import Mesh
from jax.sharding import PartitionSpec as P

GX = ("gx_0", "gx_1")
GY = ("gy_0", "gy_1")
ALL = GX + GY

EPS = 1e-06
NT = 5
ROWS = 80
TOP = 8
SPAN = 416
F32 = jnp.float32


def lanes():
    return lax.broadcasted_iota(jnp.int32, (8, 128), 1)


def from_north(tiles):
    lane = lanes()
    turned = [pltpu.roll(tile, 127, 1) for tile in tiles]
    count = len(tiles)
    return [jnp.where(lane == 127, turned[(t + 1) % count], turned[t]) for t in range(count)]


def from_south(tiles):
    lane = lanes()
    turned = [pltpu.roll(tile, 1, 1) for tile in tiles]
    count = len(tiles)
    return [jnp.where(lane == 0, turned[(t - 1) % count], turned[t]) for t in range(count)]


def at(t, start, size=8):
    return pl.ds(ROWS * t + start, size)


def tile_of(ref, layer, t, start):
    return ref[layer, at(t, start), :]


def tiles_of(ref, layer, start):
    return [tile_of(ref, layer, t, start) for t in range(NT)]


def flat_tiles(ref, start):
    return [ref[at(t, start), :] for t in range(NT)]


UNITS = 25


def strip_units(layers):
    return [(f, layer) for f in range(4) for layer in range(layers)] + [(4, None), (5, None)]


def edge_kernel(layers, par, par_x, p_in, k_in, o_in, r_in, act_in, rech_in,
                p_ref, k_ref, o_ref, r_ref, act_ref, rech_ref, send_a, send_b, act_int, sems):
    fields = (p_ref, k_ref, o_ref, r_ref)
    copies = []
    for t in (0, 3, 1, 2):
        cols = pl.ds(128 * t, 128)
        own = at(t, TOP, 64)
        for f, (src, dst) in enumerate(zip((p_in, k_in, o_in, r_in), fields)):
            copies.append(pltpu.make_async_copy(src.at[:, :, cols], dst.at[:, own, :], sems.at[t, f]))
        copies.append(pltpu.make_async_copy(act_in.at[:, cols], act_int.at[t], sems.at[t, 4]))
        copies.append(pltpu.make_async_copy(rech_in.at[:, cols], rech_ref.at[own, :], sems.at[t, 5]))
    for copy in copies:
        copy.start()
    zero = jnp.zeros((8, 128), F32)

    def clear(layer, carry):
        for ref in fields:
            for t in range(NT):
                ref[layer, at(t, 0), :] = zero
                ref[layer, at(t, ROWS - 8), :] = zero
        return carry

    lax.fori_loop(0, layers, clear, 0)
    for ref in (act_ref, rech_ref):
        for t in range(NT):
            ref[at(t, 0), :] = zero
            ref[at(t, ROWS - 8), :] = zero
    for copy in copies[:12]:
        copy.wait()
    first = lanes() < 5
    last = lanes() >= 123
    odd = par[0] == 1

    def pack(row, carry):
        rows = pl.ds(pl.multiple_of(8 * row, 8), 8)
        start = pl.multiple_of(TOP + 8 * row, 8)
        low = [zero, zero]
        high = [zero, zero]
        for u, (f, layer) in enumerate(strip_units(layers)):
            place = 5 * (u % UNITS)
            here = u // UNITS
            if f == 4:
                a, b = act_int[0, rows, :].astype(F32), act_int[3, rows, :].astype(F32)
            elif f == 5:
                a, b = rech_ref[at(0, start), :], rech_ref[at(3, start), :]
            else:
                a, b = tile_of(fields[f], layer, 0, start), tile_of(fields[f], layer, 3, start)
            a = jnp.where(first, a, 0.0)
            b = jnp.where(last, b, 0.0)
            low[here] = low[here] + (pltpu.roll(a, place, 1) if place else a)
            high[here] = high[here] + pltpu.roll(b, (place + 5) % 128, 1)
        for here in range(2):
            send_a[here, rows, :] = jnp.where(odd, low[here], high[here])
            send_b[here, rows, :] = jnp.where(odd, high[here], low[here])
        return carry

    lax.fori_loop(0, 8, pack, 0)
    for copy in copies[12:]:
        copy.wait()
    for t in range(4):
        act_ref[at(t, TOP, 64), :] = act_int[t].astype(F32)


def unpack_strips(layers, odd, got_a, got_b, rows, put):
    left_edge = lanes() >= 123
    right_edge = lanes() < 5
    a = [got_a[here, rows, :] for here in range(2)]
    b = [got_b[here, rows, :] for here in range(2)]
    below = [jnp.where(odd, a[h], b[h]) for h in range(2)]
    above = [jnp.where(odd, b[h], a[h]) for h in range(2)]
    for u, (f, layer) in enumerate(strip_units(layers)):
        place = 5 * (u % UNITS)
        here = u // UNITS
        left = pltpu.roll(below[here], (123 - place) % 128, 1)
        right = pltpu.roll(above[here], 128 - place, 1) if place else above[here]
        put(f, layer, jnp.where(left_edge, left, jnp.where(right_edge, right, 0.0)))


STRIP_ROWS = ((0, 5), (5, 5), (10, 4), (14, 4))


def turn_kernel(layers, par_y, par_x, p_ref, k_ref, o_ref, r_ref, act_ref, rech_ref, got_a, got_b,
                send_a, send_b, corners, act_corner, rech_corner):
    fields = (p_ref, k_ref, o_ref, r_ref)
    odd = par_y[0] == 1
    for side in range(2):
        def put(f, layer, value):
            if f == 4:
                act_corner[side] = value
            elif f == 5:
                rech_corner[side] = value
            else:
                corners[f, side, layer] = value

        unpack_strips(layers, odd, got_a, got_b, pl.ds(56 * side, 8), put)
    for send, side in ((send_a, 1 - par_x[0]), (send_b, par_x[0])):
        first5, first4 = 3 * side, 4 * side
        start5, start4 = TOP + 59 * side, TOP + 60 * side

        def fill(layer, carry):
            for f, (place, depth) in enumerate(STRIP_ROWS):
                start, first = (start5, first5) if depth == 5 else (start4, first4)
                rows = pl.ds(layer * 18 + place, depth)
                for t in range(4):
                    send[t, rows, :] = fields[f][layer, at(t, start, depth), :]
                send[4, rows, :] = corners[f, side, layer, pl.ds(first, depth), :]
            return carry

        lax.fori_loop(0, layers, fill, 0)
        for t in range(4):
            send[t, 18 * layers:18 * layers + 5, :] = act_ref[at(t, start5, 5), :]
            send[t, 18 * layers + 5:18 * layers + 9, :] = rech_ref[at(t, start4, 4), :]
        send[4, 18 * layers:18 * layers + 5, :] = act_corner[side, pl.ds(first5, 5), :]
        send[4, 18 * layers + 5:18 * layers + 9, :] = rech_corner[side, pl.ds(first4, 4), :]


def place_strips(layers, up, refs, got_a, got_b):
    p_ref, k_ref, o_ref, r_ref, rech_ref, act_ref = refs
    fields = (p_ref, k_ref, o_ref, r_ref)
    low, high = TOP, TOP + 64
    for got, above in ((got_a, jnp.logical_not(up)), (got_b, up)):
        dst5 = jnp.where(above, high, low - 5)
        dst4 = jnp.where(above, high, low - 4)

        def fill(layer, carry):
            for (place, depth), ref in zip(STRIP_ROWS, fields):
                start = dst5 if depth == 5 else dst4
                for t in range(NT):
                    ref[layer, at(t, start, depth), :] = got[t, pl.ds(layer * 18 + place, depth), :]
            return carry

        lax.fori_loop(0, layers, fill, 0)
        for t in range(NT):
            act_ref[at(t, dst5, 5), :] = got[t, 18 * layers:18 * layers + 5, :]
            rech_ref[at(t, dst4, 4), :] = got[t, 18 * layers + 5:18 * layers + 9, :]


def sigmoid_tile(value, layer, t, start, sig_ref, mob_ref, der_ref):
    sig = jax.nn.sigmoid(value)
    square = sig * sig
    sig_ref[layer, at(t, start), :] = sig
    mob_ref[layer, at(t, start), :] = 0.5 * square
    der_ref[layer, at(t, start), :] = square - square * sig


def face(trans, p_a, p_b, m_a, m_b, s_a, s_b, gravity):
    drop = p_a - p_b
    if gravity:
        drop = drop + gravity
    by_mob = trans * (m_a + m_b)
    by_drop = trans * drop
    return by_mob + s_a * by_drop, s_b * by_drop - by_mob, by_mob * drop


def over_layers(layers, one_layer, carry):
    if layers % 2:
        return lax.fori_loop(0, layers, one_layer, carry)
    return lax.fori_loop(0, layers // 2, lambda i, c: one_layer(2 * i + 1, one_layer(2 * i, c)), carry)


def far_faces(layers, starts, s, make_trans):
    def one_layer(layer, carry):
        upper = jnp.minimum(layer + 1, layers - 1)
        inner = jnp.where(layer + 1 < layers, 1.0, 0.0).astype(F32)
        for start in starts:
            for t in range(NT):
                here = at(t, start)
                if make_trans:
                    trans = s.ax[here, :] * (tile_of(s.k, layer, t, start) + tile_of(s.k, layer, t, start + 1))
                    s.tx[layer, here, :] = trans
                else:
                    trans = tile_of(s.tx, layer, t, start)
                p = tile_of(s.p, layer, t, start)
                m = tile_of(s.m, layer, t, start)
                der = tile_of(s.s, layer, t, start)
                ca, cb, flow = face(
                    trans, p, tile_of(s.p, layer, t, start + 1), m, tile_of(s.m, layer, t, start + 1),
                    der, tile_of(s.s, layer, t, start + 1), 0.0)
                s.xa[layer, here, :] = ca
                s.xb[layer, here, :] = cb
                s.xf[layer, here, :] = flow
                if make_trans:
                    trans = (s.act[here, :] * inner) * (
                        tile_of(s.k, layer, t, start) + tile_of(s.k, upper, t, start))
                    s.tz[layer, here, :] = trans
                else:
                    trans = tile_of(s.tz, layer, t, start)
                za, zb, zf = face(
                    trans, p, tile_of(s.p, upper, t, start), m, tile_of(s.m, upper, t, start),
                    der, tile_of(s.s, upper, t, start), -1.0)
                s.za[layer + 1, here, :] = za
                s.zb[layer + 1, here, :] = zb
                s.zf[layer + 1, here, :] = zf
        return carry

    over_layers(layers, one_layer, 0)


def y_faces(layers, starts, s, make_trans):
    def one_layer(layer, carry):
        for start in starts:
            p = tiles_of(s.p, layer, start)
            m = tiles_of(s.m, layer, start)
            der = tiles_of(s.s, layer, start)
            p_north, m_north, s_north = from_north(p), from_north(m), from_north(der)
            if make_trans:
                k = tiles_of(s.k, layer, start)
                k_north = from_north(k)
            for t in range(NT):
                here = at(t, start)
                if make_trans:
                    trans = s.ay[here, :] * (k[t] + k_north[t])
                    s.ty[layer, here, :] = trans
                else:
                    trans = tile_of(s.ty, layer, t, start)
                ca, cb, flow = face(trans, p[t], p_north[t], m[t], m_north[t], der[t], s_north[t], 0.0)
                s.ya[layer, here, :] = ca
                s.yb[layer, here, :] = cb
                s.yf[layer, here, :] = flow
        return carry

    over_layers(layers, one_layer, 0)


def assemble(layers, starts, s):
    def one_layer(layer, carry):
        for start in starts:
            ya = tiles_of(s.ya, layer, start)
            yb = tiles_of(s.yb, layer, start)
            yf = tiles_of(s.yf, layer, start)
            ya_south, yb_south, yf_south = from_south(ya), from_south(yb), from_south(yf)
            for t in range(NT):
                here = at(t, start)
                s.ya[layer, here, :] = ya_south[t]
                ap = tile_of(s.ap, layer, t, start)
                ocean = 1.0 - s.act[here, :]
                sig = tile_of(s.sig, layer, t, start)
                stored = ap * sig
                center = (stored - stored * sig) + ocean
                center = center + (tile_of(s.xa, layer, t, start) - tile_of(s.xb, layer, t, start - 1))
                center = center + (tile_of(s.za, layer + 1, t, start) - tile_of(s.zb, layer, t, start))
                s.c[layer, here, :] = center + (ya[t] - yb_south[t])
                flows = tile_of(s.xf, layer, t, start) - tile_of(s.xf, layer, t, start - 1)
                flows = flows + (tile_of(s.zf, layer + 1, t, start) - tile_of(s.zf, layer, t, start))
                flows = flows + (yf[t] - yf_south[t])
                s.q[layer, here, :] = (
                    (tile_of(s.s0, layer, t, start) - stored) - ocean * tile_of(s.p, layer, t, start) - flows)
        return carry

    over_layers(layers, one_layer, 0)


def product_tile(layers, s, v_ref, layer, start, count):
    v = tiles_of(v_ref, layer, start)
    north, south = from_north(v), from_south(v)
    upper = jnp.minimum(layer + 1, layers - 1)
    lower = jnp.maximum(layer - 1, 0)
    out = []
    for t in range(count):
        value = tile_of(s.c, layer, t, start) * v[t]
        value = value + (tile_of(s.xb, layer, t, start) * tile_of(v_ref, layer, t, start + 1)
                         - tile_of(s.xa, layer, t, start - 1) * tile_of(v_ref, layer, t, start - 1))
        value = value + (tile_of(s.yb, layer, t, start) * north[t] - tile_of(s.ya, layer, t, start) * south[t])
        value = value + (tile_of(s.zb, layer + 1, t, start) * tile_of(v_ref, upper, t, start)
                         - tile_of(s.za, layer, t, start) * tile_of(v_ref, lower, t, start))
        out.append(value)
    return v, out


def first_product(layers, starts, s):
    def one_layer(layer, carry):
        for start in starts:
            _, out = product_tile(layers, s, s.q, layer, start, NT)
            for t in range(NT):
                s.w[layer, at(t, start), :] = out[t]
        return carry

    over_layers(layers, one_layer, 0)


def second_product(layers, starts, s, sums, z_ref):
    def one_layer(layer, sums):
        sums = list(sums)
        for start in starts:
            w, z = product_tile(layers, s, s.w, layer, start, NT - 1)
            for t in range(NT - 1):
                q = tile_of(s.q, layer, t, start)
                if z_ref is not None:
                    z_ref[layer, pl.ds(64 * t + start - TOP, 8), :] = z[t]
                for i, (a, b) in enumerate(((q, q), (q, w[t]), (q, z[t]), (w[t], w[t]), (w[t], z[t]), (z[t], z[t]))):
                    sums[i] = sums[i] + a * b
        return tuple(sums)

    return over_layers(layers, one_layer, sums)


def put_sums(sums, out_ref):
    lane = lax.broadcasted_iota(jnp.int32, (1, 128), 1)
    row = jnp.zeros((1, 128), F32)
    for i, part in enumerate(sums):
        total = jnp.sum(jnp.sum(part, axis=0, keepdims=True), axis=1, keepdims=True)
        row = row + jnp.where(lane == i, total, 0.0)
    out_ref[...] = jnp.broadcast_to(row, out_ref.shape)


def step_weights(sums_ref):
    total = jnp.sum(sums_ref[...], axis=0, keepdims=True)
    lane = lax.broadcasted_iota(jnp.int32, (1, 128), 1)
    qq, qw, qz, ww, wz, zz = (
        jnp.sum(jnp.where(lane == i, total, 0.0), axis=1, keepdims=True) for i in range(6))
    first = qq + EPS
    qq, qw, qz, ww, wz, zz = (entry / first for entry in (qq, qw, qz, ww, wz, zz))
    norm = jnp.sqrt(first)
    h11 = qw
    left = jnp.maximum(ww - 2.0 * h11 * qw + h11 * h11 * qq, 0.0)
    square = left + EPS
    h21 = jnp.sqrt(square)
    h12 = (qz - h11 * qw) / h21
    h22 = (wz - h11 * qz - h11 * (ww - h11 * qw)) / square
    length = (zz - 2.0 * h11 * wz + h11 * h11 * ww) / square
    cross = (qw - h11 * qq) / h21
    rest = (length - 2.0 * (h12 * h12 + h22 * h22) + h12 * h12 * qq + h22 * h22 * (left / square)
            + 2.0 * h12 * h22 * cross)
    third = jnp.maximum(rest, 0.0) + EPS
    radius = jnp.sqrt(h11 * h11 + square)
    cosine = h11 / radius
    sine = h21 / radius
    top = cosine * h12 + sine * h22
    lower = cosine * h22 - sine * h12
    y2 = -lower * sine * norm / (lower * lower + third)
    y1 = (cosine * norm - top * y2) / radius
    b = y2 / (norm * h21)
    a = y1 / norm - b * h11
    return jnp.broadcast_to(a, (8, 128)), jnp.broadcast_to(b, (8, 128))


class Refs:
    def __init__(self, **refs):
        self.__dict__.update(refs)


STATE = ("p", "k", "s0", "ap", "tx", "ty", "tz", "q", "w")
COEFS = ("c", "xa", "xb", "ya", "yb", "za", "zb", "xf", "zf")
POINT = ("sig", "m", "s", "yf")
TALL = ("za", "zb", "zf")
PLANES = ("act", "rech", "ax", "ay")


def space(layers, name):
    return pltpu.VMEM((layers + (name in TALL), SPAN, 128), F32)


def clear_bottom(s):
    zero = jnp.zeros((8, 128), F32)

    def clear(i, carry):
        for ref in (s.za, s.zb, s.zf):
            ref[0, pl.ds(pl.multiple_of(8 * i, 8), 8), :] = zero
        return carry

    lax.fori_loop(0, SPAN // 8, clear, 0)


def mask_pairs(s, starts):
    for start in starts:
        act = flat_tiles(s.act, start)
        north = from_north(act)
        for t in range(NT):
            s.ax[at(t, start), :] = 0.5 * act[t] * s.act[at(t, start + 1), :]
            s.ay[at(t, start), :] = 0.5 * act[t] * north[t]


def points(layers, s, new, old):
    def point(layer, carry):
        top = jnp.where(layer == layers - 1, 1.0, 0.0).astype(F32)
        for start in (*new, *old):
            for t in range(NT):
                sigmoid_tile(tile_of(s.p, layer, t, start), layer, t, start, s.sig, s.m, s.s)
                if start in new:
                    act = s.act[at(t, start), :]
                    ap = (0.9 * act) * tile_of(s.ap, layer, t, start)
                    s.ap[layer, at(t, start), :] = ap
                    s.s0[layer, at(t, start), :] = (
                        ap * jax.nn.sigmoid(tile_of(s.s0, layer, t, start)) + (top * act) * s.rech[at(t, start), :])
        return carry

    lax.fori_loop(0, layers, point, 0)


def inner_kernel(layers, par_y, p_old, k_old, o_old, r_old, act_old, rech_old, got_a, got_b, after, *refs):
    names = STATE + COEFS + PLANES
    s = Refs(**dict(zip(names, refs)))
    part_ref, s.sig, s.m, s.s, s.yf = refs[len(names):]
    zero = jnp.zeros((8, 128), F32)
    fields = (s.p, s.k, s.s0, s.ap)
    clear_bottom(s)
    odd = par_y[0] == 1

    def unpack(row, carry):
        start = pl.multiple_of(TOP + 8 * row, 8)

        def put(f, layer, value):
            if f == 4:
                s.act[at(4, start), :] = value
            elif f == 5:
                s.rech[at(4, start), :] = value
            else:
                fields[f][layer, at(4, start), :] = value

        unpack_strips(layers, odd, got_a, got_b, pl.ds(pl.multiple_of(8 * row, 8), 8), put)
        return carry

    lax.fori_loop(0, 8, unpack, 0)
    points(layers, s, range(8, 72, 8), ())
    mask_pairs(s, (*range(8, 64, 8), 63))
    far_faces(layers, (*range(8, 64, 8), 63), s, True)
    y_faces(layers, range(12, 68, 8), s, True)
    assemble(layers, range(12, 68, 8), s)
    first_product(layers, range(20, 60, 8), s)
    sums = second_product(layers, range(24, 56, 8), s, (zero,) * 6, None)
    for i in range(6):
        part_ref[i] = sums[i]


def first_kernel(layers, par_x, *refs):
    names = STATE + COEFS + PLANES
    count = len(names)
    part_ref, got_a, got_b = refs[count:count + 3]
    refs = refs[count + 3:]
    s = Refs(**dict(zip(names, refs)))
    sums_ref = refs[count]
    s.sig, s.m, s.s, s.yf = refs[count + 1:]
    place_strips(layers, par_x[0] == 1, (s.p, s.k, s.s0, s.ap, s.rech, s.act), got_a, got_b)
    points(layers, s, (0, 72), (8, 64))
    mask_pairs(s, (0, 4, 64, 68))
    far_faces(layers, (0, 64, 68), s, True)
    y_faces(layers, (4, 68), s, True)
    assemble(layers, (4, 68), s)
    first_product(layers, (4, 12, 60, 68), s)
    sums = second_product(layers, (8, 16, 56, 64), s, tuple(part_ref[i] for i in range(6)), None)
    put_sums(sums, sums_ref)


KEPT = ("s0", "ap", "tx", "ty", "tz", "act")
SHARED = 4
MOVED = ("p", "q", "w") + COEFS[:SHARED]


def next_kernel(layers, *refs):
    kept, refs = refs[:len(KEPT)], refs[len(KEPT) + len(MOVED):]
    got_ref, *refs = refs
    s = Refs(**dict(zip(KEPT, kept)), **dict(zip(MOVED, refs)))
    z_ref, sums_ref, *own = refs[len(MOVED):]
    for name, ref in zip(COEFS[SHARED:] + POINT, own):
        setattr(s, name, ref)
    p_ref, q_ref, w_ref = s.p, s.q, s.w
    a, b = step_weights(got_ref)
    if SHARED < len(COEFS):
        clear_bottom(s)

    def point(layer, carry):
        for start in range(4, 76, 8):
            for t in range(NT):
                p = tile_of(p_ref, layer, t, start) + (
                    a * tile_of(q_ref, layer, t, start) + b * tile_of(w_ref, layer, t, start))
                p_ref[layer, at(t, start), :] = p
                sigmoid_tile(p, layer, t, start, s.sig, s.m, s.s)
        return carry

    lax.fori_loop(0, layers, point, 0)
    starts = range(4, 76, 8)
    far_faces(layers, (0, *starts), s, False)
    y_faces(layers, starts, s, False)
    assemble(layers, starts, s)
    first_product(layers, starts, s)
    sums = tuple(jnp.zeros((8, 128), F32) for _ in range(6))
    sums = second_product(layers, range(TOP, TOP + 64, 8), s, sums, z_ref)
    put_sums(sums, sums_ref)


def last_kernel(layers, p_ref, q_ref, w_ref, z_ref, got_ref, final_out, left_out, final_buf, left_buf, sems):
    a, b = step_weights(got_ref)
    for layer in range(layers):
        for start in range(0, 64, 8):
            for t in range(NT - 1):
                q = tile_of(q_ref, layer, t, TOP + start)
                w = tile_of(w_ref, layer, t, TOP + start)
                place = (layer, slice(start, start + 8), slice(128 * t, 128 * t + 128))
                final_buf[place] = tile_of(p_ref, layer, t, TOP + start) + (a * q + b * w)
                left_buf[place] = (q - a * w) - b * z_ref[layer, pl.ds(64 * t + start, 8), :]
        pltpu.make_async_copy(final_buf.at[layer], final_out.at[layer], sems.at[layer, 0]).start()
        pltpu.make_async_copy(left_buf.at[layer], left_out.at[layer], sems.at[layer, 1]).start()
    for layer in range(layers):
        pltpu.make_async_copy(final_buf.at[layer], final_out.at[layer], sems.at[layer, 0]).wait()
        pltpu.make_async_copy(left_buf.at[layer], left_out.at[layer], sems.at[layer, 1]).wait()


VM = pl.BlockSpec(memory_space=pltpu.VMEM)
HB = pl.BlockSpec(memory_space=pl.ANY)
SM = pl.BlockSpec(memory_space=pltpu.SMEM)


def grant(mib):
    return pltpu.CompilerParams(vmem_limit_bytes=mib * 1024 * 1024)


def keep(*arrays):
    return [pltpu.with_memory_space_constraint(array, pltpu.VMEM) for array in arrays]


def outside(*arrays):
    return [pltpu.with_memory_space_constraint(array, pltpu.HBM) for array in arrays]


def swap(value, axes, first):
    size = lax.axis_size(axes)
    pairs = [(i, i + 1) for i in range(first, size - 1, 2)]
    return lax.ppermute(value, axes, pairs + [(b, a) for a, b in pairs])


def bound(kernel, *args):
    def call(*refs):
        kernel(*args, *refs)

    return call


def body(pressure, pressure_old, conductivity, porosity, recharge, active):
    layers = pressure.shape[0]
    par_x = (lax.axis_index(GX[1]) & 1).astype(jnp.int32).reshape(1)
    par_y = (lax.axis_index(GY[1]) & 1).astype(jnp.int32).reshape(1)
    inputs = outside(pressure, conductivity, pressure_old, porosity, active, recharge)
    dma = pltpu.SemaphoreType.DMA
    strip_y = pltpu.VMEM((2, 64, 128), F32)
    strip_x = pltpu.VMEM((NT, 192, 128), F32)
    plane = pltpu.VMEM((SPAN, 128), F32)
    part = pltpu.VMEM((8, 8, 128), F32)
    block = jax.ShapeDtypeStruct((128, 128), F32)
    loaded = (space(layers, "p"),) * 4 + (plane,) * 2
    *fields, send_a, send_b = pl.pallas_call(
        bound(edge_kernel, layers), name="edge", out_shape=loaded + (strip_y,) * 2, in_specs=[SM] * 2 + [HB] * 6,
        out_specs=(VM,) * 8, scratch_shapes=[pltpu.VMEM((4, 64, 128), jnp.int32), dma((4, 6))],
        compiler_params=grant(GRANT),
    )(par_y, par_x, *inputs)
    y_a = swap(send_a, GY, 0)
    y_b = swap(send_b, GY, 1)
    send_a, send_b = pl.pallas_call(
        bound(turn_kernel, layers), name="turn", out_shape=(strip_x,) * 2, in_specs=[SM] * 2 + [VM] * 8,
        out_specs=(VM,) * 2,
        scratch_shapes=[pltpu.VMEM((4, 2, layers, 8, 128), F32), pltpu.VMEM((2, 8, 128), F32),
                        pltpu.VMEM((2, 8, 128), F32)],
        compiler_params=grant(GRANT),
    )(par_y, par_x, *keep(*fields), y_a, y_b)
    x_a = swap(send_a, GX, 0)
    x_b = swap(send_b, GX, 1)
    state = tuple(space(layers, name) for name in STATE + COEFS) + (plane,) * 4
    points_scratch = [space(layers, name) for name in POINT]
    *fields, part_sums = pl.pallas_call(
        bound(inner_kernel, layers), name="inner", out_shape=state + (part,),
        in_specs=[SM] + [VM] * 9, out_specs=(VM,) * (len(state) + 1),
        input_output_aliases={1: 0, 2: 1, 3: 2, 4: 3, 5: len(state) - 4, 6: len(state) - 3},
        scratch_shapes=points_scratch, compiler_params=grant(GRANT),
        cost_estimate=pl.CostEstimate(flops=100_000_000, transcendentals=0, bytes_accessed=6_000_000),
    )(par_y, *keep(*fields), y_a, y_b, send_a)
    *fields, sums = pl.pallas_call(
        bound(first_kernel, layers), name="first", out_shape=state + (block,),
        in_specs=[SM] + [VM] * (len(state) + 3), out_specs=(VM,) * (len(state) + 1),
        input_output_aliases={i + 1: i for i in range(len(state))},
        scratch_shapes=points_scratch, compiler_params=grant(GRANT),
    )(par_x, *keep(*fields, part_sums), x_a, x_b)
    sums = lax.all_to_all(sums, ALL, 0, 0, tiled=True)
    named = dict(zip(STATE + COEFS + PLANES, fields))
    moved = tuple(space(layers, name) for name in MOVED)
    p, q, w, *rest = pl.pallas_call(
        bound(next_kernel, layers), name="next",
        out_shape=moved + (pltpu.VMEM((layers, 256, 128), F32), block),
        in_specs=[VM] * (len(KEPT) + len(MOVED) + 1), out_specs=(VM,) * (len(MOVED) + 2),
        input_output_aliases={len(KEPT) + i: i for i in range(len(MOVED))},
        scratch_shapes=[space(layers, name) for name in COEFS[SHARED:] + POINT], compiler_params=grant(GRANT2),
    )(*keep(*(named[n] for n in KEPT + MOVED)), sums)
    z, sums = rest[-2:]
    sums = lax.all_to_all(sums, ALL, 0, 0, tiled=True)
    out = jax.ShapeDtypeStruct(pressure.shape, F32)
    buffer = pltpu.VMEM(pressure.shape, F32)
    return pl.pallas_call(
        bound(last_kernel, layers), name="last", out_shape=(out, out), in_specs=[VM] * 5, out_specs=(HB, HB),
        scratch_shapes=[buffer, buffer, dma((layers, 2))], compiler_params=grant(GRANT),
    )(*keep(p, q, w, z), sums)


GRANT = 12
GRANT2 = 22


def solution(mesh):
    torus = Mesh(mesh.devices.reshape(4, 4, 4, 2), ALL)
    field = P(None, GX, GY)
    plane = P(GX, GY)
    return jax.shard_map(
        body, mesh=torus, in_specs=(field,) * 4 + (plane,) * 2, out_specs=(field, field), check_vma=False)
```

```python
import jax
import jax.numpy as jnp
from jax import lax
from jax.experimental import pallas as pl
from jax.experimental.pallas import tpu as pltpu
from jax.sharding import Mesh
from jax.sharding import PartitionSpec as P

GX = ("gx_0", "gx_1")
GY = ("gy_0", "gy_1")
ALL = GX + GY

EPS = 1e-06
NT = 5
ROWS = 80
TOP = 8
SPAN = 416
F32 = jnp.float32


def lanes():
    return lax.broadcasted_iota(jnp.int32, (8, 128), 1)


def from_north(tiles):
    lane = lanes()
    turned = [pltpu.roll(tile, 127, 1) for tile in tiles]
    count = len(tiles)
    return [jnp.where(lane == 127, turned[(t + 1) % count], turned[t]) for t in range(count)]


def from_south(tiles):
    lane = lanes()
    turned = [pltpu.roll(tile, 1, 1) for tile in tiles]
    count = len(tiles)
    return [jnp.where(lane == 0, turned[(t - 1) % count], turned[t]) for t in range(count)]


def at(t, start, size=8):
    return pl.ds(ROWS * t + start, size)


def tile_of(ref, layer, t, start):
    return ref[layer, at(t, start), :]


def tiles_of(ref, layer, start):
    return [tile_of(ref, layer, t, start) for t in range(NT)]


def flat_tiles(ref, start):
    return [ref[at(t, start), :] for t in range(NT)]


UNITS = 25


def strip_units(layers):
    return [(f, layer) for f in range(4) for layer in range(layers)] + [(4, None), (5, None)]


def edge_kernel(layers, par, par_x, p_in, k_in, o_in, r_in, act_in, rech_in,
                p_ref, k_ref, o_ref, r_ref, act_ref, rech_ref, send_a, send_b, act_int, sems):
    fields = (p_ref, k_ref, o_ref, r_ref)
    copies = []
    for t in (0, 3, 1, 2):
        cols = pl.ds(128 * t, 128)
        own = at(t, TOP, 64)
        for f, (src, dst) in enumerate(zip((p_in, k_in, o_in, r_in), fields)):
            copies.append(pltpu.make_async_copy(src.at[:, :, cols], dst.at[:, own, :], sems.at[t, f]))
        copies.append(pltpu.make_async_copy(act_in.at[:, cols], act_int.at[t], sems.at[t, 4]))
        copies.append(pltpu.make_async_copy(rech_in.at[:, cols], rech_ref.at[own, :], sems.at[t, 5]))
    for copy in copies:
        copy.start()
    zero = jnp.zeros((8, 128), F32)

    def clear(layer, carry):
        for ref in fields:
            for t in range(NT):
                ref[layer, at(t, 0), :] = zero
                ref[layer, at(t, ROWS - 8), :] = zero
        return carry

    lax.fori_loop(0, layers, clear, 0)
    for ref in (act_ref, rech_ref):
        for t in range(NT):
            ref[at(t, 0), :] = zero
            ref[at(t, ROWS - 8), :] = zero
    for copy in copies[:12]:
        copy.wait()
    first = lanes() < 5
    last = lanes() >= 123
    odd = par[0] == 1

    def pack(row, carry):
        rows = pl.ds(pl.multiple_of(8 * row, 8), 8)
        start = pl.multiple_of(TOP + 8 * row, 8)
        low = [zero, zero]
        high = [zero, zero]
        for u, (f, layer) in enumerate(strip_units(layers)):
            place = 5 * (u % UNITS)
            here = u // UNITS
            if f == 4:
                a, b = act_int[0, rows, :].astype(F32), act_int[3, rows, :].astype(F32)
            elif f == 5:
                a, b = rech_ref[at(0, start), :], rech_ref[at(3, start), :]
            else:
                a, b = tile_of(fields[f], layer, 0, start), tile_of(fields[f], layer, 3, start)
            a = jnp.where(first, a, 0.0)
            b = jnp.where(last, b, 0.0)
            low[here] = low[here] + (pltpu.roll(a, place, 1) if place else a)
            high[here] = high[here] + pltpu.roll(b, (place + 5) % 128, 1)
        for here in range(2):
            send_a[here, rows, :] = jnp.where(odd, low[here], high[here])
            send_b[here, rows, :] = jnp.where(odd, high[here], low[here])
        return carry

    lax.fori_loop(0, 8, pack, 0)
    for copy in copies[12:]:
        copy.wait()
    for t in range(4):
        act_ref[at(t, TOP, 64), :] = act_int[t].astype(F32)


def unpack_strips(layers, odd, got_a, got_b, rows, put):
    left_edge = lanes() >= 123
    right_edge = lanes() < 5
    a = [got_a[here, rows, :] for here in range(2)]
    b = [got_b[here, rows, :] for here in range(2)]
    below = [jnp.where(odd, a[h], b[h]) for h in range(2)]
    above = [jnp.where(odd, b[h], a[h]) for h in range(2)]
    for u, (f, layer) in enumerate(strip_units(layers)):
        place = 5 * (u % UNITS)
        here = u // UNITS
        left = pltpu.roll(below[here], (123 - place) % 128, 1)
        right = pltpu.roll(above[here], 128 - place, 1) if place else above[here]
        put(f, layer, jnp.where(left_edge, left, jnp.where(right_edge, right, 0.0)))


STRIP_ROWS = ((0, 5), (5, 5), (10, 4), (14, 4))


GROUPS = 12


def turn_kernel(layers, par_y, par_x, got_a, got_b, old_a, old_b, send_a, send_b, corners, act_corner, rech_corner, flat):
    odd = par_y[0] == 1
    flat[184:192, :] = jnp.zeros((8, 128), F32)
    for side in range(2):
        def put(f, layer, value):
            if f == 4:
                act_corner[side] = value
            elif f == 5:
                rech_corner[side] = value
            else:
                corners[f, side, layer] = value

        unpack_strips(layers, odd, got_a, got_b, pl.ds(56 * side, 8), put)
    for send, side in ((send_a, 1 - par_x[0]), (send_b, par_x[0])):
        first5, first4 = 3 * side, 4 * side

        def fill(layer, carry):
            for f, (place, depth) in enumerate(STRIP_ROWS):
                first = first5 if depth == 5 else first4
                flat[pl.ds(layer * 18 + place, depth), :] = corners[f, side, layer, pl.ds(first, depth), :]
            return carry

        lax.fori_loop(0, layers, fill, 0)
        flat[18 * layers:18 * layers + 5, :] = act_corner[side, pl.ds(first5, 5), :]
        flat[18 * layers + 5:18 * layers + 9, :] = rech_corner[side, pl.ds(first4, 4), :]

        def pack(half, carry):
            rows = jnp.zeros((8, 128), F32)
            for g in range(GROUPS):
                rows = rows + pltpu.roll(flat[pl.ds(pl.multiple_of(16 * g + 8 * half, 8), 8), :], 10 * g + 5, 1)
            send[pl.ds(pl.multiple_of(768 + 8 * half, 8), 8), :] = rows
            return carry

        lax.fori_loop(0, 2, pack, 0)


def place_strips(layers, up, refs, got_a, got_b, flat):
    p_ref, k_ref, o_ref, r_ref, rech_ref, act_ref = refs
    fields = (p_ref, k_ref, o_ref, r_ref)
    low, high = TOP, TOP + 64
    lane = lanes()
    beside = (lane >= 123) | (lane < 5)
    for got, above in ((got_a, jnp.logical_not(up)), (got_b, up)):
        dst5 = jnp.where(above, high, low - 5)
        dst4 = jnp.where(above, high, low - 4)

        def unpack(half, carry):
            rows = got[pl.ds(pl.multiple_of(768 + 8 * half, 8), 8), :]
            for g in range(GROUPS):
                flat[pl.ds(pl.multiple_of(16 * g + 8 * half, 8), 8), :] = jnp.where(
                    beside, pltpu.roll(rows, 123 - 10 * g, 1), 0.0)
            return carry

        lax.fori_loop(0, 2, unpack, 0)

        def fill(layer, carry):
            for (place, depth), ref in zip(STRIP_ROWS, fields):
                start = dst5 if depth == 5 else dst4
                for t in range(4):
                    ref[layer, at(t, start, depth), :] = got[pl.ds(192 * t + layer * 18 + place, depth), :]
                ref[layer, at(4, start, depth), :] = flat[pl.ds(layer * 18 + place, depth), :]
            return carry

        lax.fori_loop(0, layers, fill, 0)
        for t in range(NT):
            rows = flat if t == 4 else got
            first = (0 if t == 4 else 192 * t) + 18 * layers
            act_ref[at(t, dst5, 5), :] = rows[first:first + 5, :]
            rech_ref[at(t, dst4, 4), :] = rows[first + 5:first + 9, :]


def sigmoid_tile(value, layer, t, start, sig_ref, mob_ref, der_ref):
    sig = jax.nn.sigmoid(value)
    square = sig * sig
    sig_ref[layer, at(t, start), :] = sig
    mob_ref[layer, at(t, start), :] = 0.5 * square
    der_ref[layer, at(t, start), :] = square - square * sig


def face(trans, p_a, p_b, m_a, m_b, s_a, s_b, gravity):
    drop = p_a - p_b
    if gravity:
        drop = drop + gravity
    by_mob = trans * (m_a + m_b)
    by_drop = trans * drop
    return by_mob + s_a * by_drop, s_b * by_drop - by_mob, by_mob * drop


def over_layers(layers, one_layer, carry):
    trip = 5 if layers % 5 == 0 else 1

    def several(i, carry):
        for layer in range(trip):
            carry = one_layer(trip * i + layer, carry)
        return carry

    return lax.fori_loop(0, layers // trip, several, carry)


def far_faces(layers, starts, s, make_trans, tiles=range(NT)):
    def one_layer(layer, carry):
        upper = jnp.minimum(layer + 1, layers - 1)
        inner = jnp.where(layer + 1 < layers, 1.0, 0.0).astype(F32)
        for start in starts:
            for t in tiles:
                here = at(t, start)
                if make_trans:
                    trans = s.ax[here, :] * (tile_of(s.k, layer, t, start) + tile_of(s.k, layer, t, start + 1))
                    s.tx[layer, here, :] = trans
                else:
                    trans = tile_of(s.tx, layer, t, start)
                p = tile_of(s.p, layer, t, start)
                m = tile_of(s.m, layer, t, start)
                der = tile_of(s.s, layer, t, start)
                ca, cb, flow = face(
                    trans, p, tile_of(s.p, layer, t, start + 1), m, tile_of(s.m, layer, t, start + 1),
                    der, tile_of(s.s, layer, t, start + 1), 0.0)
                s.xa[layer, here, :] = ca
                s.xb[layer, here, :] = cb
                s.xf[layer, here, :] = flow
                if make_trans:
                    trans = (s.act[here, :] * inner) * (
                        tile_of(s.k, layer, t, start) + tile_of(s.k, upper, t, start))
                    s.tz[layer, here, :] = trans
                else:
                    trans = tile_of(s.tz, layer, t, start)
                za, zb, zf = face(
                    trans, p, tile_of(s.p, upper, t, start), m, tile_of(s.m, upper, t, start),
                    der, tile_of(s.s, upper, t, start), -1.0)
                s.za[layer + 1, here, :] = za
                s.zb[layer + 1, here, :] = zb
                s.zf[layer + 1, here, :] = zf
        return carry

    over_layers(layers, one_layer, 0)


def y_faces(layers, starts, s, make_trans):
    def one_layer(layer, carry):
        for start in starts:
            p = tiles_of(s.p, layer, start)
            m = tiles_of(s.m, layer, start)
            der = tiles_of(s.s, layer, start)
            p_north, m_north, s_north = from_north(p), from_north(m), from_north(der)
            if make_trans:
                k = tiles_of(s.k, layer, start)
                k_north = from_north(k)
            for t in range(NT):
                here = at(t, start)
                if make_trans:
                    trans = s.ay[here, :] * (k[t] + k_north[t])
                    s.ty[layer, here, :] = trans
                else:
                    trans = tile_of(s.ty, layer, t, start)
                ca, cb, flow = face(trans, p[t], p_north[t], m[t], m_north[t], der[t], s_north[t], 0.0)
                s.ya[layer, here, :] = ca
                s.yb[layer, here, :] = cb
                s.yf[layer, here, :] = flow
        return carry

    over_layers(layers, one_layer, 0)


def assemble(layers, starts, s):
    def one_layer(layer, carry):
        for start in starts:
            ya = tiles_of(s.ya, layer, start)
            yb = tiles_of(s.yb, layer, start)
            yf = tiles_of(s.yf, layer, start)
            ya_south, yb_south, yf_south = from_south(ya), from_south(yb), from_south(yf)
            for t in range(NT):
                here = at(t, start)
                s.ya[layer, here, :] = ya_south[t]
                ap = tile_of(s.ap, layer, t, start)
                ocean = 1.0 - s.act[here, :]
                sig = tile_of(s.sig, layer, t, start)
                stored = ap * sig
                center = (stored - stored * sig) + ocean
                center = center + (tile_of(s.xa, layer, t, start) - tile_of(s.xb, layer, t, start - 1))
                center = center + (tile_of(s.za, layer + 1, t, start) - tile_of(s.zb, layer, t, start))
                s.c[layer, here, :] = center + (ya[t] - yb_south[t])
                flows = tile_of(s.xf, layer, t, start) - tile_of(s.xf, layer, t, start - 1)
                flows = flows + (tile_of(s.zf, layer + 1, t, start) - tile_of(s.zf, layer, t, start))
                flows = flows + (yf[t] - yf_south[t])
                s.q[layer, here, :] = (
                    (tile_of(s.s0, layer, t, start) - stored) - ocean * tile_of(s.p, layer, t, start) - flows)
        return carry

    over_layers(layers, one_layer, 0)


def product_tile(layers, s, v_ref, layer, start, count):
    v = tiles_of(v_ref, layer, start)
    north, south = from_north(v), from_south(v)
    upper = jnp.minimum(layer + 1, layers - 1)
    lower = jnp.maximum(layer - 1, 0)
    out = []
    for t in range(count):
        value = tile_of(s.c, layer, t, start) * v[t]
        value = value + (tile_of(s.xb, layer, t, start) * tile_of(v_ref, layer, t, start + 1)
                         - tile_of(s.xa, layer, t, start - 1) * tile_of(v_ref, layer, t, start - 1))
        value = value + (tile_of(s.yb, layer, t, start) * north[t] - tile_of(s.ya, layer, t, start) * south[t])
        value = value + (tile_of(s.zb, layer + 1, t, start) * tile_of(v_ref, upper, t, start)
                         - tile_of(s.za, layer, t, start) * tile_of(v_ref, lower, t, start))
        out.append(value)
    return v, out


def first_product(layers, starts, s):
    def one_layer(layer, carry):
        for start in starts:
            _, out = product_tile(layers, s, s.q, layer, start, NT)
            for t in range(NT):
                s.w[layer, at(t, start), :] = out[t]
        return carry

    over_layers(layers, one_layer, 0)


def second_product(layers, starts, s, sums, z_ref):
    def one_layer(layer, sums):
        sums = list(sums)
        for start in starts:
            w, z = product_tile(layers, s, s.w, layer, start, NT - 1)
            for t in range(NT - 1):
                q = tile_of(s.q, layer, t, start)
                if z_ref is not None:
                    z_ref[layer, pl.ds(64 * t + start - TOP, 8), :] = z[t]
                for i, (a, b) in enumerate(((q, q), (q, w[t]), (q, z[t]), (w[t], w[t]), (w[t], z[t]), (z[t], z[t]))):
                    sums[i] = sums[i] + a * b
        return tuple(sums)

    return over_layers(layers, one_layer, sums)


def put_sums(sums, out_ref):
    lane = lax.broadcasted_iota(jnp.int32, (1, 128), 1)
    row = jnp.zeros((1, 128), F32)
    for i, part in enumerate(sums):
        total = jnp.sum(jnp.sum(part, axis=0, keepdims=True), axis=1, keepdims=True)
        row = row + jnp.where(lane == i, total, 0.0)
    out_ref[...] = jnp.broadcast_to(row, out_ref.shape)


def step_weights(sums_ref):
    total = jnp.sum(sums_ref[...], axis=0, keepdims=True)
    lane = lax.broadcasted_iota(jnp.int32, (1, 128), 1)
    qq, qw, qz, ww, wz, zz = (
        jnp.sum(jnp.where(lane == i, total, 0.0), axis=1, keepdims=True) for i in range(6))
    first = qq + EPS
    qq, qw, qz, ww, wz, zz = (entry / first for entry in (qq, qw, qz, ww, wz, zz))
    norm = jnp.sqrt(first)
    h11 = qw
    left = jnp.maximum(ww - 2.0 * h11 * qw + h11 * h11 * qq, 0.0)
    square = left + EPS
    h21 = jnp.sqrt(square)
    h12 = (qz - h11 * qw) / h21
    h22 = (wz - h11 * qz - h11 * (ww - h11 * qw)) / square
    length = (zz - 2.0 * h11 * wz + h11 * h11 * ww) / square
    cross = (qw - h11 * qq) / h21
    rest = (length - 2.0 * (h12 * h12 + h22 * h22) + h12 * h12 * qq + h22 * h22 * (left / square)
            + 2.0 * h12 * h22 * cross)
    third = jnp.maximum(rest, 0.0) + EPS
    radius = jnp.sqrt(h11 * h11 + square)
    cosine = h11 / radius
    sine = h21 / radius
    top = cosine * h12 + sine * h22
    lower = cosine * h22 - sine * h12
    y2 = -lower * sine * norm / (lower * lower + third)
    y1 = (cosine * norm - top * y2) / radius
    b = y2 / (norm * h21)
    a = y1 / norm - b * h11
    return jnp.broadcast_to(a, (8, 128)), jnp.broadcast_to(b, (8, 128))


class Refs:
    def __init__(self, **refs):
        self.__dict__.update(refs)


STATE = ("p", "k", "s0", "ap", "tx", "ty", "tz", "q", "w")
COEFS = ("c", "xa", "xb", "ya", "yb", "za", "zb", "xf", "zf")
POINT = ("sig", "m", "s")
TALL = ("za", "zb", "zf")
PLANES = ("act", "rech", "ax", "ay")


def space(layers, name):
    return pltpu.VMEM((layers + (name in TALL), SPAN, 128), F32)


def clear_bottom(s):
    zero = jnp.zeros((8, 128), F32)

    def clear(i, carry):
        for ref in (s.za, s.zb, s.zf):
            ref[0, pl.ds(pl.multiple_of(8 * i, 8), 8), :] = zero
        return carry

    lax.fori_loop(0, SPAN // 8, clear, 0)


def mask_pairs_x(s, starts, tiles=range(NT)):
    for start in starts:
        for t in tiles:
            s.ax[at(t, start), :] = 0.5 * s.act[at(t, start), :] * s.act[at(t, start + 1), :]


def mask_pairs_y(s, starts):
    for start in starts:
        act = flat_tiles(s.act, start)
        north = from_north(act)
        for t in range(NT):
            s.ay[at(t, start), :] = 0.5 * act[t] * north[t]


def points(layers, s, new, old, tiles=range(NT)):
    def point(layer, carry):
        top = jnp.where(layer == layers - 1, 1.0, 0.0).astype(F32)
        for start in (*new, *old):
            for t in tiles:
                sigmoid_tile(tile_of(s.p, layer, t, start), layer, t, start, s.sig, s.m, s.s)
                if start in new:
                    act = s.act[at(t, start), :]
                    ap = (0.9 * act) * tile_of(s.ap, layer, t, start)
                    s.ap[layer, at(t, start), :] = ap
                    s.s0[layer, at(t, start), :] = (
                        ap * jax.nn.sigmoid(tile_of(s.s0, layer, t, start)) + (top * act) * s.rech[at(t, start), :])
        return carry

    lax.fori_loop(0, layers, point, 0)


OWN_ROWS = range(TOP, TOP + 64, 8)
FACE_ROWS = (*range(TOP, TOP + 56, 8), TOP + 55)


def before_kernel(layers, par_x, p_old, k_old, o_old, r_old, act_old, rech_old, *refs):
    names = STATE + COEFS + PLANES + POINT
    s = Refs(**dict(zip(names, refs)))
    send_a, send_b = refs[len(names):]
    fields = (s.p, s.k, s.s0, s.ap)
    for send, side in ((send_a, 1 - par_x[0]), (send_b, par_x[0])):
        start5, start4 = TOP + 59 * side, TOP + 60 * side

        def fill(layer, carry):
            for f, (place, depth) in enumerate(STRIP_ROWS):
                start = start5 if depth == 5 else start4
                for t in range(4):
                    send[pl.ds(192 * t + layer * 18 + place, depth), :] = fields[f][layer, at(t, start, depth), :]
            return carry

        lax.fori_loop(0, layers, fill, 0)
        for t in range(4):
            send[pl.ds(192 * t + 18 * layers, 5), :] = s.act[at(t, start5, 5), :]
            send[pl.ds(192 * t + 18 * layers + 5, 4), :] = s.rech[at(t, start4, 4), :]
    clear_bottom(s)
    points(layers, s, OWN_ROWS, (), range(4))
    mask_pairs_x(s, FACE_ROWS, range(4))
    far_faces(layers, FACE_ROWS, s, True, range(4))


def inner_kernel(layers, par_y, got_a, got_b, after, *refs):
    names = STATE + COEFS + PLANES + POINT
    refs = refs[len(names):]
    s = Refs(**dict(zip(names, refs)))
    part_ref, s.yf = refs[len(names):]
    zero = jnp.zeros((8, 128), F32)
    fields = (s.p, s.k, s.s0, s.ap)
    odd = par_y[0] == 1

    def unpack(row, carry):
        start = pl.multiple_of(TOP + 8 * row, 8)

        def put(f, layer, value):
            if f == 4:
                s.act[at(4, start), :] = value
            elif f == 5:
                s.rech[at(4, start), :] = value
            else:
                fields[f][layer, at(4, start), :] = value

        unpack_strips(layers, odd, got_a, got_b, pl.ds(pl.multiple_of(8 * row, 8), 8), put)
        return carry

    lax.fori_loop(0, 8, unpack, 0)
    points(layers, s, OWN_ROWS, (), (4,))
    mask_pairs_x(s, FACE_ROWS, (4,))
    mask_pairs_y(s, FACE_ROWS)
    far_faces(layers, FACE_ROWS, s, True, (4,))
    y_faces(layers, range(12, 68, 8), s, True)
    assemble(layers, range(12, 68, 8), s)
    first_product(layers, (13, 21, 29, 37, 45, 53, 59), s)
    sums = second_product(layers, range(16, 64, 8), s, (zero,) * 6, None)
    for i in range(6):
        part_ref[i] = sums[i]


def first_kernel(layers, par_x, *refs):
    names = STATE + COEFS + PLANES + POINT
    count = len(names)
    part_ref, got_a, got_b = refs[count:count + 3]
    refs = refs[count + 3:]
    s = Refs(**dict(zip(names, refs)))
    sums_ref = refs[count]
    s.yf, flat = refs[count + 1:]
    place_strips(layers, par_x[0] == 1, (s.p, s.k, s.s0, s.ap, s.rech, s.act), got_a, got_b, flat)
    points(layers, s, (0, 72), (8, 64))
    mask_pairs_x(s, (0, 4, 64, 68))
    mask_pairs_y(s, (0, 4, 64, 68))
    far_faces(layers, (0, 64, 68), s, True)
    y_faces(layers, (4, 68), s, True)
    assemble(layers, (4, 68), s)
    first_product(layers, (5, 67), s)
    sums = second_product(layers, (8, 64), s, tuple(part_ref[i] for i in range(6)), None)
    put_sums(sums, sums_ref)


KEPT = ("s0", "ap", "tx", "ty", "tz", "act")
SHARED = 8
MOVED = ("p", "q", "w") + POINT + COEFS[:SHARED]


def next_kernel(layers, *refs):
    kept, refs = refs[:len(KEPT)], refs[len(KEPT) + len(MOVED):]
    got_ref, *refs = refs
    s = Refs(**dict(zip(KEPT, kept)), **dict(zip(MOVED, refs)))
    z_ref, sums_ref, *own = refs[len(MOVED):]
    for name, ref in zip(COEFS[SHARED:] + ("yf",), own):
        setattr(s, name, ref)
    p_ref, q_ref, w_ref = s.p, s.q, s.w
    a, b = step_weights(got_ref)
    if SHARED < len(COEFS):
        clear_bottom(s)

    def point(layer, carry):
        for start in range(4, 76, 8):
            for t in range(NT):
                p = tile_of(p_ref, layer, t, start) + (
                    a * tile_of(q_ref, layer, t, start) + b * tile_of(w_ref, layer, t, start))
                p_ref[layer, at(t, start), :] = p
                sigmoid_tile(p, layer, t, start, s.sig, s.m, s.s)
        return carry

    lax.fori_loop(0, layers, point, 0)
    far_faces(layers, range(5, 77, 8), s, False)
    starts = range(6, 78, 8)
    y_faces(layers, starts, s, False)
    assemble(layers, starts, s)
    first_product(layers, starts, s)
    sums = tuple(jnp.zeros((8, 128), F32) for _ in range(6))
    sums = second_product(layers, range(TOP, TOP + 64, 8), s, sums, z_ref)
    put_sums(sums, sums_ref)


def last_kernel(layers, p_ref, q_ref, w_ref, z_ref, got_ref, final_out, left_out, final_buf, left_buf, sems):
    a, b = step_weights(got_ref)
    for layer in range(layers):
        for start in range(0, 64, 8):
            for t in range(NT - 1):
                q = tile_of(q_ref, layer, t, TOP + start)
                w = tile_of(w_ref, layer, t, TOP + start)
                place = (layer, slice(start, start + 8), slice(128 * t, 128 * t + 128))
                final_buf[place] = tile_of(p_ref, layer, t, TOP + start) + (a * q + b * w)
                left_buf[place] = (q - a * w) - b * z_ref[layer, pl.ds(64 * t + start, 8), :]
        pltpu.make_async_copy(final_buf.at[layer], final_out.at[layer], sems.at[layer, 0]).start()
        pltpu.make_async_copy(left_buf.at[layer], left_out.at[layer], sems.at[layer, 1]).start()
    for layer in range(layers):
        pltpu.make_async_copy(final_buf.at[layer], final_out.at[layer], sems.at[layer, 0]).wait()
        pltpu.make_async_copy(left_buf.at[layer], left_out.at[layer], sems.at[layer, 1]).wait()


VM = pl.BlockSpec(memory_space=pltpu.VMEM)
HB = pl.BlockSpec(memory_space=pl.ANY)
SM = pl.BlockSpec(memory_space=pltpu.SMEM)


def grant(mib):
    return pltpu.CompilerParams(vmem_limit_bytes=mib * 1024 * 1024)


def keep(*arrays):
    return [pltpu.with_memory_space_constraint(array, pltpu.VMEM) for array in arrays]


def outside(*arrays):
    return [pltpu.with_memory_space_constraint(array, pltpu.HBM) for array in arrays]


def swap(value, axes, first):
    size = lax.axis_size(axes)
    pairs = [(i, i + 1) for i in range(first, size - 1, 2)]
    return lax.ppermute(value, axes, pairs + [(b, a) for a, b in pairs])


def bound(kernel, *args):
    def call(*refs):
        kernel(*args, *refs)

    return call


def body(pressure, pressure_old, conductivity, porosity, recharge, active):
    layers = pressure.shape[0]
    par_x = (lax.axis_index(GX[1]) & 1).astype(jnp.int32).reshape(1)
    par_y = (lax.axis_index(GY[1]) & 1).astype(jnp.int32).reshape(1)
    inputs = outside(pressure, conductivity, pressure_old, porosity, active, recharge)
    dma = pltpu.SemaphoreType.DMA
    strip_y = pltpu.VMEM((2, 64, 128), F32)
    strip_x = pltpu.VMEM((784, 128), F32)
    rows_x = pltpu.VMEM((192, 128), F32)
    plane = pltpu.VMEM((SPAN, 128), F32)
    part = pltpu.VMEM((8, 8, 128), F32)
    block = jax.ShapeDtypeStruct((128, 128), F32)
    loaded = (space(layers, "p"),) * 4 + (plane,) * 2
    *fields, send_a, send_b = pl.pallas_call(
        bound(edge_kernel, layers), name="edge", out_shape=loaded + (strip_y,) * 2, in_specs=[SM] * 2 + [HB] * 6,
        out_specs=(VM,) * 8, scratch_shapes=[pltpu.VMEM((4, 64, 128), jnp.int32), dma((4, 6))],
        compiler_params=grant(GRANT),
    )(par_y, par_x, *inputs)
    y_a = swap(send_a, GY, 0)
    y_b = swap(send_b, GY, 1)
    state = tuple(space(layers, name) for name in STATE + COEFS) + (plane,) * 4 + tuple(space(layers, n) for n in POINT)
    count = len(state)
    act_at = len(STATE + COEFS)
    flow = space(layers, "yf")
    *fields, send_a, send_b = pl.pallas_call(
        bound(before_kernel, layers), name="before", out_shape=state + (strip_x,) * 2,
        in_specs=[SM] + [VM] * 6, out_specs=(VM,) * (count + 2),
        input_output_aliases={1: 0, 2: 1, 3: 2, 4: 3, 5: act_at, 6: act_at + 1}, compiler_params=grant(GRANT),
        cost_estimate=pl.CostEstimate(flops=20_000_000, transcendentals=0, bytes_accessed=6_000_000),
    )(par_x, *keep(*fields))
    send_a, send_b = pl.pallas_call(
        bound(turn_kernel, layers), name="turn", out_shape=(strip_x,) * 2, in_specs=[SM] * 2 + [VM] * 4,
        out_specs=(VM,) * 2, input_output_aliases={4: 0, 5: 1},
        scratch_shapes=[pltpu.VMEM((4, 2, layers, 8, 128), F32), pltpu.VMEM((2, 8, 128), F32),
                        pltpu.VMEM((2, 8, 128), F32), rows_x],
        compiler_params=grant(GRANT),
    )(par_y, par_x, y_a, y_b, *keep(send_a, send_b))
    x_a = swap(send_a, GX, 0)
    x_b = swap(send_b, GX, 1)
    *fields, part_sums = pl.pallas_call(
        bound(inner_kernel, layers), name="inner", out_shape=state + (part,),
        in_specs=[SM] + [VM] * (3 + count), out_specs=(VM,) * (count + 1),
        input_output_aliases={i + 4: i for i in range(count)},
        scratch_shapes=[flow], compiler_params=grant(GRANT),
        cost_estimate=pl.CostEstimate(flops=100_000_000, transcendentals=0, bytes_accessed=6_000_000),
    )(par_y, y_a, y_b, send_a, *keep(*fields))
    *fields, sums = pl.pallas_call(
        bound(first_kernel, layers), name="first", out_shape=state + (block,),
        in_specs=[SM] + [VM] * (count + 3), out_specs=(VM,) * (count + 1),
        input_output_aliases={i + 1: i for i in range(count)},
        scratch_shapes=[flow, rows_x], compiler_params=grant(GRANT),
    )(par_x, *keep(*fields, part_sums), x_a, x_b)
    sums = lax.all_to_all(sums, ALL, 0, 0, tiled=True)
    named = dict(zip(STATE + COEFS + PLANES + POINT, fields))
    moved = tuple(space(layers, name) for name in MOVED)
    p, q, w, *rest = pl.pallas_call(
        bound(next_kernel, layers), name="next",
        out_shape=moved + (pltpu.VMEM((layers, 256, 128), F32), block),
        in_specs=[VM] * (len(KEPT) + len(MOVED) + 1), out_specs=(VM,) * (len(MOVED) + 2),
        input_output_aliases={len(KEPT) + i: i for i in range(len(MOVED))},
        scratch_shapes=[space(layers, name) for name in COEFS[SHARED:] + ("yf",)], compiler_params=grant(GRANT2),
    )(*keep(*(named[n] for n in KEPT + MOVED)), sums)
    z, sums = rest[-2:]
    sums = lax.all_to_all(sums, ALL, 0, 0, tiled=True)
    out = jax.ShapeDtypeStruct(pressure.shape, F32)
    buffer = pltpu.VMEM(pressure.shape, F32)
    return pl.pallas_call(
        bound(last_kernel, layers), name="last", out_shape=(out, out), in_specs=[VM] * 5, out_specs=(HB, HB),
        scratch_shapes=[buffer, buffer, dma((layers, 2))], compiler_params=grant(GRANT),
    )(*keep(p, q, w, z), sums)


GRANT = 6
GRANT2 = 8


def solution(mesh):
    torus = Mesh(mesh.devices.reshape(4, 4, 4, 2), ALL)
    field = P(None, GX, GY)
    plane = P(GX, GY)
    return jax.shard_map(
        body, mesh=torus, in_specs=(field,) * 4 + (plane,) * 2, out_specs=(field, field), check_vma=False)
```

```python
import jax
import jax.numpy as jnp
from jax import lax
from jax.experimental import pallas as pl
from jax.experimental.pallas import tpu as pltpu
from jax.sharding import Mesh
from jax.sharding import PartitionSpec as P

GX = ("gx_0", "gx_1")
GY = ("gy_0", "gy_1")
ALL = GX + GY

EPS = 1e-06
NT = 5
ROWS = 80
TOP = 8
SPAN = 416
F32 = jnp.float32


def lanes():
    return lax.broadcasted_iota(jnp.int32, (8, 128), 1)


def from_north(tiles):
    lane = lanes()
    turned = [pltpu.roll(tile, 127, 1) for tile in tiles]
    count = len(tiles)
    return [jnp.where(lane == 127, turned[(t + 1) % count], turned[t]) for t in range(count)]


def from_south(tiles):
    lane = lanes()
    turned = [pltpu.roll(tile, 1, 1) for tile in tiles]
    count = len(tiles)
    return [jnp.where(lane == 0, turned[(t - 1) % count], turned[t]) for t in range(count)]


def at(t, start, size=8):
    return pl.ds(ROWS * t + start, size)


def tile_of(ref, layer, t, start):
    return ref[layer, at(t, start), :]


def tiles_of(ref, layer, start):
    return [tile_of(ref, layer, t, start) for t in range(NT)]


def flat_tiles(ref, start):
    return [ref[at(t, start), :] for t in range(NT)]


UNITS = 25


def strip_units(layers):
    return [(f, layer) for f in range(4) for layer in range(layers)] + [(4, None), (5, None)]


def edge_kernel(layers, par, par_x, p_in, k_in, o_in, r_in, act_in, rech_in,
                p_ref, k_ref, o_ref, r_ref, act_ref, rech_ref, send_a, send_b, act_int, sems):
    fields = (p_ref, k_ref, o_ref, r_ref)
    copies = []
    for t in (0, 3):
        cols = pl.ds(128 * t, 128)
        own = at(t, TOP, 64)
        for f, (src, dst) in enumerate(zip((p_in, k_in, o_in, r_in), fields)):
            copies.append(pltpu.make_async_copy(src.at[:, :, cols], dst.at[:, own, :], sems.at[t, f]))
        copies.append(pltpu.make_async_copy(act_in.at[:, cols], act_int.at[t], sems.at[t, 4]))
        copies.append(pltpu.make_async_copy(rech_in.at[:, cols], rech_ref.at[own, :], sems.at[t, 5]))
    for copy in copies:
        copy.start()
    zero = jnp.zeros((8, 128), F32)

    def clear(layer, carry):
        for ref in fields:
            for t in range(NT):
                ref[layer, at(t, 0), :] = zero
                ref[layer, at(t, ROWS - 8), :] = zero
        return carry

    lax.fori_loop(0, layers, clear, 0)
    for ref in (act_ref, rech_ref):
        for t in range(NT):
            ref[at(t, 0), :] = zero
            ref[at(t, ROWS - 8), :] = zero
    for copy in copies:
        copy.wait()
    first = lanes() < 5
    last = lanes() >= 123
    odd = par[0] == 1

    def pack(row, carry):
        rows = pl.ds(pl.multiple_of(8 * row, 8), 8)
        start = pl.multiple_of(TOP + 8 * row, 8)
        low = [zero, zero]
        high = [zero, zero]
        for u, (f, layer) in enumerate(strip_units(layers)):
            place = 5 * (u % UNITS)
            here = u // UNITS
            if f == 4:
                a, b = act_int[0, rows, :].astype(F32), act_int[3, rows, :].astype(F32)
            elif f == 5:
                a, b = rech_ref[at(0, start), :], rech_ref[at(3, start), :]
            else:
                a, b = tile_of(fields[f], layer, 0, start), tile_of(fields[f], layer, 3, start)
            a = jnp.where(first, a, 0.0)
            b = jnp.where(last, b, 0.0)
            low[here] = low[here] + (pltpu.roll(a, place, 1) if place else a)
            high[here] = high[here] + pltpu.roll(b, (place + 5) % 128, 1)
        for here in range(2):
            send_a[here, rows, :] = jnp.where(odd, low[here], high[here])
            send_b[here, rows, :] = jnp.where(odd, high[here], low[here])
        return carry

    lax.fori_loop(0, 8, pack, 0)
    for t in (0, 3):
        act_ref[at(t, TOP, 64), :] = act_int[t].astype(F32)


def unpack_strips(layers, odd, got_a, got_b, rows, put):
    left_edge = lanes() >= 123
    right_edge = lanes() < 5
    a = [got_a[here, rows, :] for here in range(2)]
    b = [got_b[here, rows, :] for here in range(2)]
    below = [jnp.where(odd, a[h], b[h]) for h in range(2)]
    above = [jnp.where(odd, b[h], a[h]) for h in range(2)]
    for u, (f, layer) in enumerate(strip_units(layers)):
        place = 5 * (u % UNITS)
        here = u // UNITS
        left = pltpu.roll(below[here], (123 - place) % 128, 1)
        right = pltpu.roll(above[here], 128 - place, 1) if place else above[here]
        put(f, layer, jnp.where(left_edge, left, jnp.where(right_edge, right, 0.0)))


STRIP_ROWS = ((0, 5), (5, 5), (10, 4), (14, 4))


GROUPS = 12


def turn_kernel(layers, par_y, par_x, got_a, got_b, old_a, old_b, send_a, send_b, corners, act_corner, rech_corner, flat):
    odd = par_y[0] == 1
    flat[184:192, :] = jnp.zeros((8, 128), F32)
    for side in range(2):
        def put(f, layer, value):
            if f == 4:
                act_corner[side] = value
            elif f == 5:
                rech_corner[side] = value
            else:
                corners[f, side, layer] = value

        unpack_strips(layers, odd, got_a, got_b, pl.ds(56 * side, 8), put)
    for send, side in ((send_a, 1 - par_x[0]), (send_b, par_x[0])):
        first5, first4 = 3 * side, 4 * side

        def fill(layer, carry):
            for f, (place, depth) in enumerate(STRIP_ROWS):
                first = first5 if depth == 5 else first4
                flat[pl.ds(layer * 18 + place, depth), :] = corners[f, side, layer, pl.ds(first, depth), :]
            return carry

        lax.fori_loop(0, layers, fill, 0)
        flat[18 * layers:18 * layers + 5, :] = act_corner[side, pl.ds(first5, 5), :]
        flat[18 * layers + 5:18 * layers + 9, :] = rech_corner[side, pl.ds(first4, 4), :]

        def pack(half, carry):
            rows = jnp.zeros((8, 128), F32)
            for g in range(GROUPS):
                rows = rows + pltpu.roll(flat[pl.ds(pl.multiple_of(16 * g + 8 * half, 8), 8), :], 10 * g + 5, 1)
            send[pl.ds(pl.multiple_of(768 + 8 * half, 8), 8), :] = rows
            return carry

        lax.fori_loop(0, 2, pack, 0)


def place_strips(layers, up, refs, got_a, got_b, flat):
    p_ref, k_ref, o_ref, r_ref, rech_ref, act_ref = refs
    fields = (p_ref, k_ref, o_ref, r_ref)
    low, high = TOP, TOP + 64
    lane = lanes()
    beside = (lane >= 123) | (lane < 5)
    for got, above in ((got_a, jnp.logical_not(up)), (got_b, up)):
        dst5 = jnp.where(above, high, low - 5)
        dst4 = jnp.where(above, high, low - 4)

        def unpack(half, carry):
            rows = got[pl.ds(pl.multiple_of(768 + 8 * half, 8), 8), :]
            for g in range(GROUPS):
                flat[pl.ds(pl.multiple_of(16 * g + 8 * half, 8), 8), :] = jnp.where(
                    beside, pltpu.roll(rows, 123 - 10 * g, 1), 0.0)
            return carry

        lax.fori_loop(0, 2, unpack, 0)

        def fill(layer, carry):
            for (place, depth), ref in zip(STRIP_ROWS, fields):
                start = dst5 if depth == 5 else dst4
                for t in range(4):
                    ref[layer, at(t, start, depth), :] = got[pl.ds(192 * t + layer * 18 + place, depth), :]
                ref[layer, at(4, start, depth), :] = flat[pl.ds(layer * 18 + place, depth), :]
            return carry

        lax.fori_loop(0, layers, fill, 0)
        for t in range(NT):
            rows = flat if t == 4 else got
            first = (0 if t == 4 else 192 * t) + 18 * layers
            act_ref[at(t, dst5, 5), :] = rows[first:first + 5, :]
            rech_ref[at(t, dst4, 4), :] = rows[first + 5:first + 9, :]


def sigmoid_tile(value, layer, t, start, sig_ref, mob_ref, der_ref):
    sig = jax.nn.sigmoid(value)
    square = sig * sig
    sig_ref[layer, at(t, start), :] = sig
    mob_ref[layer, at(t, start), :] = 0.5 * square
    der_ref[layer, at(t, start), :] = square - square * sig


def face(trans, p_a, p_b, m_a, m_b, s_a, s_b, gravity):
    drop = p_a - p_b
    if gravity:
        drop = drop + gravity
    by_mob = trans * (m_a + m_b)
    by_drop = trans * drop
    return by_mob + s_a * by_drop, s_b * by_drop - by_mob, by_mob * drop


def over_layers(layers, one_layer, carry):
    trip = 5 if layers % 5 == 0 else 1

    def several(i, carry):
        for layer in range(trip):
            carry = one_layer(trip * i + layer, carry)
        return carry

    return lax.fori_loop(0, layers // trip, several, carry)


def far_faces(layers, starts, s, make_trans, tiles=range(NT)):
    def one_layer(layer, carry):
        upper = jnp.minimum(layer + 1, layers - 1)
        inner = jnp.where(layer + 1 < layers, 1.0, 0.0).astype(F32)
        for start in starts:
            for t in tiles:
                here = at(t, start)
                if make_trans:
                    trans = s.ax[here, :] * (tile_of(s.k, layer, t, start) + tile_of(s.k, layer, t, start + 1))
                    s.tx[layer, here, :] = trans
                else:
                    trans = tile_of(s.tx, layer, t, start)
                p = tile_of(s.p, layer, t, start)
                m = tile_of(s.m, layer, t, start)
                der = tile_of(s.s, layer, t, start)
                ca, cb, flow = face(
                    trans, p, tile_of(s.p, layer, t, start + 1), m, tile_of(s.m, layer, t, start + 1),
                    der, tile_of(s.s, layer, t, start + 1), 0.0)
                s.xa[layer, here, :] = ca
                s.xb[layer, here, :] = cb
                s.xf[layer, here, :] = flow
                if make_trans:
                    trans = (s.act[here, :] * inner) * (
                        tile_of(s.k, layer, t, start) + tile_of(s.k, upper, t, start))
                    s.tz[layer, here, :] = trans
                else:
                    trans = tile_of(s.tz, layer, t, start)
                za, zb, zf = face(
                    trans, p, tile_of(s.p, upper, t, start), m, tile_of(s.m, upper, t, start),
                    der, tile_of(s.s, upper, t, start), -1.0)
                s.za[layer + 1, here, :] = za
                s.zb[layer + 1, here, :] = zb
                s.zf[layer + 1, here, :] = zf
        return carry

    over_layers(layers, one_layer, 0)


def y_faces(layers, starts, s, make_trans):
    def one_layer(layer, carry):
        for start in starts:
            p = tiles_of(s.p, layer, start)
            m = tiles_of(s.m, layer, start)
            der = tiles_of(s.s, layer, start)
            p_north, m_north, s_north = from_north(p), from_north(m), from_north(der)
            if make_trans:
                k = tiles_of(s.k, layer, start)
                k_north = from_north(k)
            for t in range(NT):
                here = at(t, start)
                if make_trans:
                    trans = s.ay[here, :] * (k[t] + k_north[t])
                    s.ty[layer, here, :] = trans
                else:
                    trans = tile_of(s.ty, layer, t, start)
                ca, cb, flow = face(trans, p[t], p_north[t], m[t], m_north[t], der[t], s_north[t], 0.0)
                s.ya[layer, here, :] = ca
                s.yb[layer, here, :] = cb
                s.yf[layer, here, :] = flow
        return carry

    over_layers(layers, one_layer, 0)


def assemble(layers, starts, s):
    def one_layer(layer, carry):
        for start in starts:
            ya = tiles_of(s.ya, layer, start)
            yb = tiles_of(s.yb, layer, start)
            yf = tiles_of(s.yf, layer, start)
            ya_south, yb_south, yf_south = from_south(ya), from_south(yb), from_south(yf)
            for t in range(NT):
                here = at(t, start)
                s.ya[layer, here, :] = ya_south[t]
                ap = tile_of(s.ap, layer, t, start)
                ocean = 1.0 - s.act[here, :]
                sig = tile_of(s.sig, layer, t, start)
                stored = ap * sig
                center = (stored - stored * sig) + ocean
                center = center + (tile_of(s.xa, layer, t, start) - tile_of(s.xb, layer, t, start - 1))
                center = center + (tile_of(s.za, layer + 1, t, start) - tile_of(s.zb, layer, t, start))
                s.c[layer, here, :] = center + (ya[t] - yb_south[t])
                flows = tile_of(s.xf, layer, t, start) - tile_of(s.xf, layer, t, start - 1)
                flows = flows + (tile_of(s.zf, layer + 1, t, start) - tile_of(s.zf, layer, t, start))
                flows = flows + (yf[t] - yf_south[t])
                s.q[layer, here, :] = (
                    (tile_of(s.s0, layer, t, start) - stored) - ocean * tile_of(s.p, layer, t, start) - flows)
        return carry

    over_layers(layers, one_layer, 0)


def product_tile(layers, s, v_ref, layer, start, count):
    v = tiles_of(v_ref, layer, start)
    north, south = from_north(v), from_south(v)
    upper = jnp.minimum(layer + 1, layers - 1)
    lower = jnp.maximum(layer - 1, 0)
    out = []
    for t in range(count):
        value = tile_of(s.c, layer, t, start) * v[t]
        value = value + (tile_of(s.xb, layer, t, start) * tile_of(v_ref, layer, t, start + 1)
                         - tile_of(s.xa, layer, t, start - 1) * tile_of(v_ref, layer, t, start - 1))
        value = value + (tile_of(s.yb, layer, t, start) * north[t] - tile_of(s.ya, layer, t, start) * south[t])
        value = value + (tile_of(s.zb, layer + 1, t, start) * tile_of(v_ref, upper, t, start)
                         - tile_of(s.za, layer, t, start) * tile_of(v_ref, lower, t, start))
        out.append(value)
    return v, out


def first_product(layers, starts, s):
    def one_layer(layer, carry):
        for start in starts:
            _, out = product_tile(layers, s, s.q, layer, start, NT)
            for t in range(NT):
                s.w[layer, at(t, start), :] = out[t]
        return carry

    over_layers(layers, one_layer, 0)


def second_product(layers, starts, s, sums, z_ref):
    def one_layer(layer, sums):
        sums = list(sums)
        for start in starts:
            w, z = product_tile(layers, s, s.w, layer, start, NT - 1)
            for t in range(NT - 1):
                q = tile_of(s.q, layer, t, start)
                if z_ref is not None:
                    z_ref[layer, pl.ds(64 * t + start - TOP, 8), :] = z[t]
                for i, (a, b) in enumerate(((q, q), (q, w[t]), (q, z[t]), (w[t], w[t]), (w[t], z[t]), (z[t], z[t]))):
                    sums[i] = sums[i] + a * b
        return tuple(sums)

    return over_layers(layers, one_layer, sums)


def put_sums(sums, out_ref):
    lane = lax.broadcasted_iota(jnp.int32, (1, 128), 1)
    row = jnp.zeros((1, 128), F32)
    for i, part in enumerate(sums):
        total = jnp.sum(jnp.sum(part, axis=0, keepdims=True), axis=1, keepdims=True)
        row = row + jnp.where(lane == i, total, 0.0)
    out_ref[...] = jnp.broadcast_to(row, out_ref.shape)


def step_weights(sums_ref):
    total = jnp.sum(sums_ref[...], axis=0, keepdims=True)
    lane = lax.broadcasted_iota(jnp.int32, (1, 128), 1)
    qq, qw, qz, ww, wz, zz = (
        jnp.sum(jnp.where(lane == i, total, 0.0), axis=1, keepdims=True) for i in range(6))
    first = qq + EPS
    qq, qw, qz, ww, wz, zz = (entry / first for entry in (qq, qw, qz, ww, wz, zz))
    norm = jnp.sqrt(first)
    h11 = qw
    left = jnp.maximum(ww - 2.0 * h11 * qw + h11 * h11 * qq, 0.0)
    square = left + EPS
    h21 = jnp.sqrt(square)
    h12 = (qz - h11 * qw) / h21
    h22 = (wz - h11 * qz - h11 * (ww - h11 * qw)) / square
    length = (zz - 2.0 * h11 * wz + h11 * h11 * ww) / square
    cross = (qw - h11 * qq) / h21
    rest = (length - 2.0 * (h12 * h12 + h22 * h22) + h12 * h12 * qq + h22 * h22 * (left / square)
            + 2.0 * h12 * h22 * cross)
    third = jnp.maximum(rest, 0.0) + EPS
    radius = jnp.sqrt(h11 * h11 + square)
    cosine = h11 / radius
    sine = h21 / radius
    top = cosine * h12 + sine * h22
    lower = cosine * h22 - sine * h12
    y2 = -lower * sine * norm / (lower * lower + third)
    y1 = (cosine * norm - top * y2) / radius
    b = y2 / (norm * h21)
    a = y1 / norm - b * h11
    return jnp.broadcast_to(a, (8, 128)), jnp.broadcast_to(b, (8, 128))


class Refs:
    def __init__(self, **refs):
        self.__dict__.update(refs)


STATE = ("p", "k", "s0", "ap", "tx", "ty", "tz", "q", "w")
COEFS = ("c", "xa", "xb", "ya", "yb", "za", "zb", "xf", "zf")
POINT = ("sig", "m", "s")
TALL = ("za", "zb", "zf")
PLANES = ("act", "rech", "ax", "ay")


def space(layers, name):
    return pltpu.VMEM((layers + (name in TALL), SPAN, 128), F32)


def clear_bottom(s):
    zero = jnp.zeros((8, 128), F32)

    def clear(i, carry):
        for ref in (s.za, s.zb, s.zf):
            ref[0, pl.ds(pl.multiple_of(8 * i, 8), 8), :] = zero
        return carry

    lax.fori_loop(0, SPAN // 8, clear, 0)


def mask_pairs_x(s, starts, tiles=range(NT)):
    for start in starts:
        for t in tiles:
            s.ax[at(t, start), :] = 0.5 * s.act[at(t, start), :] * s.act[at(t, start + 1), :]


def mask_pairs_y(s, starts):
    for start in starts:
        act = flat_tiles(s.act, start)
        north = from_north(act)
        for t in range(NT):
            s.ay[at(t, start), :] = 0.5 * act[t] * north[t]


def points(layers, s, new, old, tiles=range(NT)):
    def point(layer, carry):
        top = jnp.where(layer == layers - 1, 1.0, 0.0).astype(F32)
        for start in (*new, *old):
            for t in tiles:
                sigmoid_tile(tile_of(s.p, layer, t, start), layer, t, start, s.sig, s.m, s.s)
                if start in new:
                    act = s.act[at(t, start), :]
                    ap = (0.9 * act) * tile_of(s.ap, layer, t, start)
                    s.ap[layer, at(t, start), :] = ap
                    s.s0[layer, at(t, start), :] = (
                        ap * jax.nn.sigmoid(tile_of(s.s0, layer, t, start)) + (top * act) * s.rech[at(t, start), :])
        return carry

    lax.fori_loop(0, layers, point, 0)


OWN_ROWS = range(TOP, TOP + 64, 8)
FACE_ROWS = (*range(TOP, TOP + 56, 8), TOP + 55)


def before_kernel(layers, par_x, p_in, k_in, o_in, r_in, act_in, rech_in, p_old, k_old, o_old, r_old, act_old, rech_old, *refs):
    names = STATE + COEFS + PLANES + POINT
    s = Refs(**dict(zip(names, refs)))
    send_a, send_b, act_int, sems = refs[len(names):]
    fields = (s.p, s.k, s.s0, s.ap)
    copies = []
    for t in (1, 2):
        cols = pl.ds(128 * t, 128)
        own = at(t, TOP, 64)
        for f, (src, dst) in enumerate(zip((p_in, k_in, o_in, r_in), fields)):
            copies.append(pltpu.make_async_copy(src.at[:, :, cols], dst.at[:, own, :], sems.at[t - 1, f]))
        copies.append(pltpu.make_async_copy(act_in.at[:, cols], act_int.at[t - 1], sems.at[t - 1, 4]))
        copies.append(pltpu.make_async_copy(rech_in.at[:, cols], s.rech.at[own, :], sems.at[t - 1, 5]))
    for copy in copies:
        copy.start()
    clear_bottom(s)

    def pack(tiles):
        for send, side in ((send_a, 1 - par_x[0]), (send_b, par_x[0])):
            start5, start4 = TOP + 59 * side, TOP + 60 * side

            def fill(layer, carry):
                for f, (place, depth) in enumerate(STRIP_ROWS):
                    start = start5 if depth == 5 else start4
                    for t in tiles:
                        send[pl.ds(192 * t + layer * 18 + place, depth), :] = fields[f][layer, at(t, start, depth), :]
                return carry

            lax.fori_loop(0, layers, fill, 0)
            for t in tiles:
                send[pl.ds(192 * t + 18 * layers, 5), :] = s.act[at(t, start5, 5), :]
                send[pl.ds(192 * t + 18 * layers + 5, 4), :] = s.rech[at(t, start4, 4), :]

    for tiles in ((0, 3), (1, 2)):
        if tiles == (1, 2):
            for copy in copies:
                copy.wait()
            for t in tiles:
                s.act[at(t, TOP, 64), :] = act_int[t - 1].astype(F32)
        pack(tiles)
        points(layers, s, OWN_ROWS, (), tiles)
        mask_pairs_x(s, FACE_ROWS, tiles)
        far_faces(layers, FACE_ROWS, s, True, tiles)


def inner_kernel(layers, par_y, got_a, got_b, after, *refs):
    names = STATE + COEFS + PLANES + POINT
    refs = refs[len(names):]
    s = Refs(**dict(zip(names, refs)))
    part_ref, s.yf = refs[len(names):]
    zero = jnp.zeros((8, 128), F32)
    fields = (s.p, s.k, s.s0, s.ap)
    odd = par_y[0] == 1

    def unpack(row, carry):
        start = pl.multiple_of(TOP + 8 * row, 8)

        def put(f, layer, value):
            if f == 4:
                s.act[at(4, start), :] = value
            elif f == 5:
                s.rech[at(4, start), :] = value
            else:
                fields[f][layer, at(4, start), :] = value

        unpack_strips(layers, odd, got_a, got_b, pl.ds(pl.multiple_of(8 * row, 8), 8), put)
        return carry

    lax.fori_loop(0, 8, unpack, 0)
    points(layers, s, OWN_ROWS, (), (4,))
    mask_pairs_x(s, FACE_ROWS, (4,))
    mask_pairs_y(s, FACE_ROWS)
    far_faces(layers, FACE_ROWS, s, True, (4,))
    y_faces(layers, range(12, 68, 8), s, True)
    assemble(layers, range(12, 68, 8), s)
    first_product(layers, (13, 21, 29, 37, 45, 53, 59), s)
    sums = second_product(layers, range(16, 64, 8), s, (zero,) * 6, None)
    for i in range(6):
        part_ref[i] = sums[i]


def first_kernel(layers, par_x, *refs):
    names = STATE + COEFS + PLANES + POINT
    count = len(names)
    part_ref, got_a, got_b = refs[count:count + 3]
    refs = refs[count + 3:]
    s = Refs(**dict(zip(names, refs)))
    sums_ref = refs[count]
    s.yf, flat = refs[count + 1:]
    place_strips(layers, par_x[0] == 1, (s.p, s.k, s.s0, s.ap, s.rech, s.act), got_a, got_b, flat)
    points(layers, s, (0, 72), (8, 64))
    mask_pairs_x(s, (0, 4, 64, 68))
    mask_pairs_y(s, (0, 4, 64, 68))
    far_faces(layers, (0, 64, 68), s, True)
    y_faces(layers, (4, 68), s, True)
    assemble(layers, (4, 68), s)
    first_product(layers, (5, 67), s)
    sums = second_product(layers, (8, 64), s, tuple(part_ref[i] for i in range(6)), None)
    put_sums(sums, sums_ref)


KEPT = ("s0", "ap", "tx", "ty", "tz", "act")
SHARED = 8
MOVED = ("p", "q", "w") + POINT + COEFS[:SHARED]


def next_kernel(layers, *refs):
    kept, refs = refs[:len(KEPT)], refs[len(KEPT) + len(MOVED):]
    got_ref, *refs = refs
    s = Refs(**dict(zip(KEPT, kept)), **dict(zip(MOVED, refs)))
    z_ref, sums_ref, *own = refs[len(MOVED):]
    for name, ref in zip(COEFS[SHARED:] + ("yf",), own):
        setattr(s, name, ref)
    p_ref, q_ref, w_ref = s.p, s.q, s.w
    a, b = step_weights(got_ref)
    if SHARED < len(COEFS):
        clear_bottom(s)

    def point(layer, carry):
        for start in range(4, 76, 8):
            for t in range(NT):
                p = tile_of(p_ref, layer, t, start) + (
                    a * tile_of(q_ref, layer, t, start) + b * tile_of(w_ref, layer, t, start))
                p_ref[layer, at(t, start), :] = p
                sigmoid_tile(p, layer, t, start, s.sig, s.m, s.s)
        return carry

    lax.fori_loop(0, layers, point, 0)
    far_faces(layers, range(5, 77, 8), s, False)
    starts = range(6, 78, 8)
    y_faces(layers, starts, s, False)
    assemble(layers, starts, s)
    first_product(layers, starts, s)
    sums = tuple(jnp.zeros((8, 128), F32) for _ in range(6))
    sums = second_product(layers, range(TOP, TOP + 64, 8), s, sums, z_ref)
    put_sums(sums, sums_ref)


def last_kernel(layers, p_ref, q_ref, w_ref, z_ref, got_ref, final_out, left_out, final_buf, left_buf, sems):
    a, b = step_weights(got_ref)
    for layer in range(layers):
        for start in range(0, 64, 8):
            for t in range(NT - 1):
                q = tile_of(q_ref, layer, t, TOP + start)
                w = tile_of(w_ref, layer, t, TOP + start)
                place = (layer, slice(start, start + 8), slice(128 * t, 128 * t + 128))
                final_buf[place] = tile_of(p_ref, layer, t, TOP + start) + (a * q + b * w)
                left_buf[place] = (q - a * w) - b * z_ref[layer, pl.ds(64 * t + start, 8), :]
        pltpu.make_async_copy(final_buf.at[layer], final_out.at[layer], sems.at[layer, 0]).start()
        pltpu.make_async_copy(left_buf.at[layer], left_out.at[layer], sems.at[layer, 1]).start()
    for layer in range(layers):
        pltpu.make_async_copy(final_buf.at[layer], final_out.at[layer], sems.at[layer, 0]).wait()
        pltpu.make_async_copy(left_buf.at[layer], left_out.at[layer], sems.at[layer, 1]).wait()


VM = pl.BlockSpec(memory_space=pltpu.VMEM)
HB = pl.BlockSpec(memory_space=pl.ANY)
SM = pl.BlockSpec(memory_space=pltpu.SMEM)


def grant(mib):
    return pltpu.CompilerParams(vmem_limit_bytes=mib * 1024 * 1024)


def keep(*arrays):
    return [pltpu.with_memory_space_constraint(array, pltpu.VMEM) for array in arrays]


def outside(*arrays):
    return [pltpu.with_memory_space_constraint(array, pltpu.HBM) for array in arrays]


def swap(value, axes, first):
    size = lax.axis_size(axes)
    pairs = [(i, i + 1) for i in range(first, size - 1, 2)]
    return lax.ppermute(value, axes, pairs + [(b, a) for a, b in pairs])


def bound(kernel, *args):
    def call(*refs):
        kernel(*args, *refs)

    return call


def body(pressure, pressure_old, conductivity, porosity, recharge, active):
    layers = pressure.shape[0]
    par_x = (lax.axis_index(GX[1]) & 1).astype(jnp.int32).reshape(1)
    par_y = (lax.axis_index(GY[1]) & 1).astype(jnp.int32).reshape(1)
    inputs = outside(pressure, conductivity, pressure_old, porosity, active, recharge)
    dma = pltpu.SemaphoreType.DMA
    strip_y = pltpu.VMEM((2, 64, 128), F32)
    strip_x = pltpu.VMEM((784, 128), F32)
    rows_x = pltpu.VMEM((192, 128), F32)
    plane = pltpu.VMEM((SPAN, 128), F32)
    part = pltpu.VMEM((8, 8, 128), F32)
    block = jax.ShapeDtypeStruct((128, 128), F32)
    loaded = (space(layers, "p"),) * 4 + (plane,) * 2
    *fields, send_a, send_b = pl.pallas_call(
        bound(edge_kernel, layers), name="edge", out_shape=loaded + (strip_y,) * 2, in_specs=[SM] * 2 + [HB] * 6,
        out_specs=(VM,) * 8, scratch_shapes=[pltpu.VMEM((4, 64, 128), jnp.int32), dma((4, 6))],
        compiler_params=grant(GRANT),
    )(par_y, par_x, *inputs)
    y_a = swap(send_a, GY, 0)
    y_b = swap(send_b, GY, 1)
    state = tuple(space(layers, name) for name in STATE + COEFS) + (plane,) * 4 + tuple(space(layers, n) for n in POINT)
    count = len(state)
    act_at = len(STATE + COEFS)
    flow = space(layers, "yf")
    *fields, send_a, send_b = pl.pallas_call(
        bound(before_kernel, layers), name="before", out_shape=state + (strip_x,) * 2,
        in_specs=[SM] + [HB] * 6 + [VM] * 6, out_specs=(VM,) * (count + 2),
        input_output_aliases={7: 0, 8: 1, 9: 2, 10: 3, 11: act_at, 12: act_at + 1},
        scratch_shapes=[pltpu.VMEM((2, 64, 128), jnp.int32), dma((2, 6))], compiler_params=grant(GRANT),
        cost_estimate=pl.CostEstimate(flops=20_000_000, transcendentals=0, bytes_accessed=6_000_000),
    )(par_x, *inputs, *keep(*fields))
    send_a, send_b = pl.pallas_call(
        bound(turn_kernel, layers), name="turn", out_shape=(strip_x,) * 2, in_specs=[SM] * 2 + [VM] * 4,
        out_specs=(VM,) * 2, input_output_aliases={4: 0, 5: 1},
        scratch_shapes=[pltpu.VMEM((4, 2, layers, 8, 128), F32), pltpu.VMEM((2, 8, 128), F32),
                        pltpu.VMEM((2, 8, 128), F32), rows_x],
        compiler_params=grant(GRANT),
    )(par_y, par_x, y_a, y_b, *keep(send_a, send_b))
    x_a = swap(send_a, GX, 0)
    x_b = swap(send_b, GX, 1)
    *fields, part_sums = pl.pallas_call(
        bound(inner_kernel, layers), name="inner", out_shape=state + (part,),
        in_specs=[SM] + [VM] * (3 + count), out_specs=(VM,) * (count + 1),
        input_output_aliases={i + 4: i for i in range(count)},
        scratch_shapes=[flow], compiler_params=grant(GRANT),
        cost_estimate=pl.CostEstimate(flops=100_000_000, transcendentals=0, bytes_accessed=6_000_000),
    )(par_y, y_a, y_b, send_a, *keep(*fields))
    *fields, sums = pl.pallas_call(
        bound(first_kernel, layers), name="first", out_shape=state + (block,),
        in_specs=[SM] + [VM] * (count + 3), out_specs=(VM,) * (count + 1),
        input_output_aliases={i + 1: i for i in range(count)},
        scratch_shapes=[flow, rows_x], compiler_params=grant(GRANT),
    )(par_x, *keep(*fields, part_sums), x_a, x_b)
    sums = lax.all_to_all(sums, ALL, 0, 0, tiled=True)
    named = dict(zip(STATE + COEFS + PLANES + POINT, fields))
    moved = tuple(space(layers, name) for name in MOVED)
    p, q, w, *rest = pl.pallas_call(
        bound(next_kernel, layers), name="next",
        out_shape=moved + (pltpu.VMEM((layers, 256, 128), F32), block),
        in_specs=[VM] * (len(KEPT) + len(MOVED) + 1), out_specs=(VM,) * (len(MOVED) + 2),
        input_output_aliases={len(KEPT) + i: i for i in range(len(MOVED))},
        scratch_shapes=[space(layers, name) for name in COEFS[SHARED:] + ("yf",)], compiler_params=grant(GRANT2),
    )(*keep(*(named[n] for n in KEPT + MOVED)), sums)
    z, sums = rest[-2:]
    sums = lax.all_to_all(sums, ALL, 0, 0, tiled=True)
    out = jax.ShapeDtypeStruct(pressure.shape, F32)
    buffer = pltpu.VMEM(pressure.shape, F32)
    return pl.pallas_call(
        bound(last_kernel, layers), name="last", out_shape=(out, out), in_specs=[VM] * 5, out_specs=(HB, HB),
        scratch_shapes=[buffer, buffer, dma((layers, 2))], compiler_params=grant(GRANT),
    )(*keep(p, q, w, z), sums)


GRANT = 6
GRANT2 = 8


def solution(mesh):
    torus = Mesh(mesh.devices.reshape(4, 4, 4, 2), ALL)
    field = P(None, GX, GY)
    plane = P(GX, GY)
    return jax.shard_map(
        body, mesh=torus, in_specs=(field,) * 4 + (plane,) * 2, out_specs=(field, field), check_vma=False)
```
